256 devices in a mesh: slab: 64 (over y, z, x_hi), load: 4 (over x_lo, core).
Axes of the slice: x: 4 (x_hi: 2, x_lo: 2; x = x_hi * 2 + x_lo), y: 4, z: 8, core: 2. Of those that a mesh axis runs over, the one named last changes fastest.
Arguments:
- start_disp: float32 [8, 3, 64, 64, 128], P('load', None, 'slab'), may hold values from -10 to 10
- density: float32 [64, 64, 128], P('slab'), may hold values from 0.05 to 1
- design: int32 [64, 64, 128], P('slab'), may hold values from 0 to 1, as said below
- support: int32 [64, 64, 128], P('slab'), may hold values 0 or 1
- load_nodes: int32 [8, 2048], P('load'), may hold values from 0 to 524287
- load_forces: float32 [8, 3, 2048], P('load'), may hold values from -6 to 6
Outputs:
- displacement: float32 [8, 3, 64, 64, 128], P('load', None, 'slab')
- new_density: float32 [64, 64, 128], P('slab')
The draws below stay inside these ranges and needn't reach their ends.
Inputs may be any that keep to these rules, and one draw needn't show every extreme that they name: 1 marks an element of the design domain, 0 a void element; at least one element is in the design domain. `support`: 1 marks a node held fixed. `load_nodes`: flat node index z * 64 * 128 + x * 128 + y; a node may carry several forces of one load case.
All inputs are finite; a program needn't handle non-finite values. No bound on the sum of `support` on one device may be relied on, other than what follows from the above.
Results may differ from the reference program's by a relative error of at most 0.00024.
Values sent between devices are 32-bit elements; how exact they have to be, the bound alone decides.
A program may use at most 64 MiB of HBM per device.

```python
import jax
import jax.numpy as jnp
import numpy as np
from jax import lax

NX = 64
NY = 128
LOADS = 8
POINTS = 2048
SWEEPS = 4
NZ = 64
RADIUS = 2


def draw_start_disp(key, part):
    full_shape = (LOADS, 3, NZ, NX, NY)
    depth_frac = lax.broadcasted_iota(jnp.float32, full_shape, 2) / max(NZ - 1, 1)
    values = jax.random.normal(key, full_shape, jnp.float32) * jnp.sqrt(1.0 + 2.0 * depth_frac)
    return jnp.clip(values, -10.0, 10.0)


def draw_design(key, part):
    full_shape = (NZ, NX, NY)
    layer_index = lax.broadcasted_iota(jnp.int32, full_shape, 0)
    threshold = 300 + 600 * layer_index // max(NZ - 1, 1)
    return (jax.random.randint(key, full_shape, 0, 1000) < threshold).astype(jnp.int32)


def with_ends(values, rng, smallest, largest):
    place = [jax.random.randint(jax.random.fold_in(rng, axis), (), 0, length) for axis, length in enumerate(values.shape)]
    widest = values.shape.index(max(values.shape))
    neighbour = place[:widest] + [(place[widest] + 1) % values.shape[widest]] + place[widest + 1:]
    return values.at[tuple(place)].set(smallest).at[tuple(neighbour)].set(largest)


def level_of(rng, dims, split, least, high):
    def one(axis_at, blocks):
        steps = jax.random.uniform(jax.random.fold_in(jax.random.fold_in(rng, 6), axis_at), (blocks,), jnp.float32, least / len(split), high / len(split))
        return jnp.repeat(jnp.exp(steps), dims[axis_at] // blocks).reshape((-1,) + (1,) * (len(dims) - axis_at - 1))

    loudness = one(*split[0])
    for cut in split[1:]:
        loudness = loudness * one(*cut)
    return loudness


def bell_draw(stream_key, shape, width, limit, shards=(), held_as=jnp.bfloat16):
    factor_of = level_of(stream_key, shape, shards, -0.22, 0.18) if shards else 1.0
    values = jax.random.normal(stream_key, shape, jnp.float32) * width * factor_of
    return jnp.minimum(jnp.maximum(values, -limit), limit).astype(held_as)


def setup_inputs(seed: int = 0) -> dict:
    splits = jax.random.split(jax.random.key(seed), 7)
    return {
        "start_disp": draw_start_disp(jax.random.fold_in(splits[6], 71), 0),
        "density": jnp.clip(0.05 + 0.95 * jax.random.uniform(splits[1], (NZ, NX, NY), jnp.float32) ** level_of(splits[1], (NZ, NX, NY), ((0, 64),), -0.2, 0.2), 0.05, 1.0),
        "design": draw_design(jax.random.fold_in(splits[6], 71), 0),
        "support": with_ends((jax.random.randint(splits[3], (NZ, NX, NY), 0, 16) < 1).astype(jnp.int32), jax.random.fold_in(splits[3], 1), 0, 1),
        "load_nodes": with_ends(jax.random.randint(splits[4], (LOADS, POINTS), 0, NZ * NX * NY), jax.random.fold_in(splits[4], 1), 0, (NZ * NX * NY) - 1).astype(jnp.int32),
        "load_forces": bell_draw(splits[5], (LOADS, 3, POINTS), 1.0, 6.0, ((0, 4),), jnp.float32),
    }


POISSON = 0.3
STIFF_VOID = 0.001
UPPER_FACTOR = 1.2
LOWER_RATIO = 0.1
MOVE_LIMIT = 0.2
VOLUME_TARGET = 0.5
EPSILON = 1e-06
HIGHEST = lax.Precision.HIGHEST

def hex_stiffness():
    lame_first = POISSON / ((1 + POISSON) * (1 - 2 * POISSON))
    lame_shear = 1 / (2 * (1 + POISSON))
    elastic = np.zeros((6, 6))
    elastic[:3, :3] = lame_first
    for axis_a in range(3):
        elastic[axis_a, axis_a] += 2 * lame_shear
        elastic[3 + axis_a, 3 + axis_a] = lame_shear
    shear_pairs = ((0, 1), (1, 2), (0, 2))
    gauss_point = 1 / np.sqrt(3)
    matrix = np.zeros((24, 24))
    for quad_index in range(8):
        quad_coords = [gauss_point * (2 * (quad_index >> 2 - axis_a & 1) - 1) for axis_a in range(3)]
        shape_grads = np.zeros((8, 3))
        for corner in range(8):
            corner_signs = [2 * (corner >> 2 - axis_a & 1) - 1 for axis_a in range(3)]
            for axis_a in range(3):
                deriv_value = float(corner_signs[axis_a])
                for axis_b in range(3):
                    if axis_b != axis_a:
                        deriv_value *= (1 + corner_signs[axis_b] * quad_coords[axis_b]) / 2
                shape_grads[corner, axis_a] = deriv_value
        strain = np.zeros((6, 24))
        for corner in range(8):
            for axis_a in range(3):
                strain[axis_a, 3 * corner + axis_a] = shape_grads[corner, axis_a]
            for pair_index, shear_pair in enumerate(shear_pairs):
                strain[3 + pair_index, 3 * corner + shear_pair[0]] = shape_grads[corner, shear_pair[1]]
                strain[3 + pair_index, 3 * corner + shear_pair[1]] = shape_grads[corner, shear_pair[0]]
        matrix += strain.T @ elastic @ strain / 8
    return matrix.astype(np.float32)

def ahead(field, axis):
    length = field.shape[axis]
    zero_shape = list(field.shape)
    zero_shape[axis] = 1
    inner_part = lax.slice_in_dim(field, 1, length, axis=axis)
    return jnp.concatenate([inner_part, jnp.zeros(zero_shape, field.dtype)], axis)

def behind(field, axis):
    length = field.shape[axis]
    zero_shape = list(field.shape)
    zero_shape[axis] = 1
    inner_part = lax.slice_in_dim(field, 0, length - 1, axis=axis)
    return jnp.concatenate([jnp.zeros(zero_shape, field.dtype), inner_part], axis)

def corner_block(bottom, top):
    corner_parts = []
    for corner in range(8):
        corner_part = top if corner >> 2 & 1 else bottom
        if corner >> 1 & 1:
            corner_part = ahead(corner_part, corner_part.ndim - 2)
        if corner & 1:
            corner_part = ahead(corner_part, corner_part.ndim - 1)
        corner_parts.append(corner_part)
    stacked = jnp.stack(corner_parts, -4)
    return stacked.reshape(stacked.shape[:-4] + (24, stacked.shape[-2] * stacked.shape[-1]))

def spread_block(forces, rows_x, cols_y):
    shaped = forces.reshape(forces.shape[:-2] + (8, 3, rows_x, cols_y))
    to_bottom = jnp.zeros(shaped.shape[:-4] + (3, rows_x, cols_y), jnp.float32)
    to_top = to_bottom
    for corner in range(8):
        corner_part = shaped[..., corner, :, :, :]
        if corner >> 1 & 1:
            corner_part = behind(corner_part, corner_part.ndim - 2)
        if corner & 1:
            corner_part = behind(corner_part, corner_part.ndim - 1)
        if corner >> 2 & 1:
            to_top = to_top + corner_part
        else:
            to_bottom = to_bottom + corner_part
    return (to_bottom, to_top)

def gauss_table(count):
    offsets = (lax.broadcasted_iota(jnp.int32, (count, count), 0) - lax.broadcasted_iota(jnp.int32, (count, count), 1)).astype(jnp.float32)
    return jnp.exp(-(offsets / RADIUS) ** 2)

def smooth_plane(field, table_x, table_y):
    mixed = jnp.einsum('zab,ia->zib', field, table_x, precision=HIGHEST)
    return jnp.einsum('zib,jb->zij', mixed, table_y, precision=HIGHEST)

def reference(start_disp, density, design, support, load_nodes, load_forces):
    stiff_table = hex_stiffness()
    kmatrix = jnp.asarray(stiff_table)
    diag_entry = float(stiff_table[0, 0])
    design_mask = design.astype(jnp.float32)
    fixed_mask = support.astype(jnp.float32)
    free_mask = 1.0 - fixed_mask
    solid_part = design_mask * density
    stiffness = STIFF_VOID + (1.0 - STIFF_VOID) * solid_part ** 3
    beside_all = stiffness + behind(stiffness, 0)
    beside_all = beside_all + behind(beside_all, 1)
    beside_all = beside_all + behind(beside_all, 2)
    diagonal = (free_mask * diag_entry * beside_all + fixed_mask)[:, None]
    free_nodes = free_mask[:, None]
    fixed_nodes = fixed_mask[:, None]
    stiff_flat = stiffness.reshape(NZ, 1, NX * NY)

    def apply_stiffness(nodes):
        corner_vals = corner_block(nodes, ahead(nodes, 0))
        forces = jnp.einsum('ab,zbn->zan', kmatrix, corner_vals, precision=HIGHEST) * stiff_flat
        to_bottom, to_top = spread_block(forces, NX, NY)
        return to_bottom + behind(to_top, 0)

    def operate(nodes):
        return free_nodes * apply_stiffness(free_nodes * nodes) + fixed_nodes * nodes

    def solve_one(running, inputs):
        initial, indices, values = inputs
        initial = jnp.transpose(initial, (1, 0, 2, 3))
        right_side = jnp.zeros((3, NZ * NX * NY), jnp.float32).at[:, indices].add(values)
        right_side = jnp.transpose(right_side.reshape(3, NZ, NX, NY), (1, 0, 2, 3)) * free_nodes
        residual = right_side - operate(initial)
        precond = residual / diagonal
        applied = operate(precond)
        upper_bound = UPPER_FACTOR * jnp.sum(precond * applied) / jnp.sum(precond * residual)
        lower_bound = LOWER_RATIO * upper_bound
        center = 0.5 * (upper_bound + lower_bound)
        half_width = 0.5 * (upper_bound - lower_bound)
        spread_ratio = center / half_width
        factor = 1.0 / spread_ratio
        update = precond / center
        solution = initial
        for sweep_index in range(SWEEPS):
            solution = solution + update
            if sweep_index < SWEEPS - 1:
                if sweep_index == 0:
                    product = applied / center
                else:
                    product = operate(update)
                residual = residual - product
                factor_next = 1.0 / (2.0 * spread_ratio - factor)
                update = factor_next * factor * update + 2.0 * factor_next / half_width * (residual / diagonal)
                factor = factor_next
        free_part = free_nodes * solution
        corner_vals = corner_block(free_part, ahead(free_part, 0))
        forces = jnp.einsum('ab,zbn->zan', kmatrix, corner_vals, precision=HIGHEST)
        energy = lax.optimization_barrier(jnp.sum(corner_vals * forces, axis=1)).reshape(NZ, NX, NY)
        return (running + energy, jnp.transpose(solution, (1, 0, 2, 3)))
    energy_sum, displacement = lax.scan(solve_one, jnp.zeros((NZ, NX, NY), jnp.float32), (start_disp, load_nodes, load_forces))
    numer = density * (3.0 * (1.0 - STIFF_VOID)) * solid_part ** 2 * energy_sum
    table_x = gauss_table(NX)
    table_y = gauss_table(NY)
    table_z = gauss_table(NZ)

    def smooth(field):
        plane = smooth_plane(field, table_x, table_y)
        return jnp.einsum('kz,zij->kij', table_z, plane, precision=HIGHEST)
    filtered = smooth(numer) / smooth(density)
    weighted = design_mask * filtered
    count = jnp.sum(design_mask)
    ratio = weighted / (jnp.sum(weighted) / count + EPSILON)
    trial = jnp.clip(density * jnp.sqrt(ratio), density - MOVE_LIMIT, density + MOVE_LIMIT)
    scale = VOLUME_TARGET / (jnp.sum(design_mask * trial) / count + EPSILON)
    new_density = design_mask * jnp.minimum(scale * trial, 1.0)
    return (displacement, new_density)
```

```python
import jax
import jax.numpy as jnp
import numpy as np
from jax import lax
from jax.experimental import pallas as pl
from jax.experimental.pallas import tpu as pltpu
from jax.sharding import PartitionSpec as P

SWEEPS = 4
RADIUS = 2
POISSON = 0.3
STIFF_VOID = 0.001
UPPER_FACTOR = 1.2
LOWER_RATIO = 0.1
MOVE_LIMIT = 0.2
VOLUME_TARGET = 0.5
EPSILON = 1e-06
HIGHEST = lax.Precision.HIGHEST
MESH = pl.DeviceIdType.MESH
F32 = jnp.float32

NY_, NZ_ = 4, 8
LOADS_AX = 4
RING = 2 * LOADS_AX
PLANE = NY_ * NZ_
ROWS, COLS = 64, 128
POINTS = 2048
CHUNK = 256


def hex_stiffness():
    lame_first = POISSON / ((1 + POISSON) * (1 - 2 * POISSON))
    lame_shear = 1 / (2 * (1 + POISSON))
    elastic = np.zeros((6, 6))
    elastic[:3, :3] = lame_first
    for axis_a in range(3):
        elastic[axis_a, axis_a] += 2 * lame_shear
        elastic[3 + axis_a, 3 + axis_a] = lame_shear
    shear_pairs = ((0, 1), (1, 2), (0, 2))
    gauss_point = 1 / np.sqrt(3)
    matrix = np.zeros((24, 24))
    for quad_index in range(8):
        quad_coords = [
            gauss_point * (2 * (quad_index >> 2 - axis_a & 1) - 1) for axis_a in range(3)
        ]
        shape_grads = np.zeros((8, 3))
        for corner in range(8):
            corner_signs = [2 * (corner >> 2 - axis_a & 1) - 1 for axis_a in range(3)]
            for axis_a in range(3):
                deriv_value = float(corner_signs[axis_a])
                for axis_b in range(3):
                    if axis_b != axis_a:
                        deriv_value *= (1 + corner_signs[axis_b] * quad_coords[axis_b]) / 2
                shape_grads[corner, axis_a] = deriv_value
        strain = np.zeros((6, 24))
        for corner in range(8):
            for axis_a in range(3):
                strain[axis_a, 3 * corner + axis_a] = shape_grads[corner, axis_a]
            for pair_index, shear_pair in enumerate(shear_pairs):
                strain[3 + pair_index, 3 * corner + shear_pair[0]] = shape_grads[
                    corner, shear_pair[1]
                ]
                strain[3 + pair_index, 3 * corner + shear_pair[1]] = shape_grads[
                    corner, shear_pair[0]
                ]
        matrix += strain.T @ elastic @ strain / 8
    return matrix.astype(np.float32)


def mode_stiffness():
    ke = hex_stiffness().astype(np.float64)
    w = np.zeros((24, 24))
    for p in range(8):
        for o in range(8):
            sign = 1.0
            for a in range(3):
                if p >> (2 - a) & 1:
                    sign *= 1.0 if o >> (2 - a) & 1 else -1.0
            for c in range(3):
                w[3 * p + c, 3 * o + c] = sign
    return w @ ke @ w.T / 64


KHAT = mode_stiffness()
KD = float(hex_stiffness()[0, 0])


def kh(p, c, q, d):
    return float(KHAT[3 * p + c, 3 * q + d])


SHEAR = kh(1, 0, 1, 0)
TRACE = kh(1, 2, 2, 1)
NORMAL = kh(1, 2, 1, 2) - TRACE
TWIST = kh(3, 0, 5, 1)
BEND = kh(3, 1, 3, 1)
CROSS = kh(3, 1, 5, 0)
LAST = kh(7, 0, 7, 0)

SHEAR_PAIRS = (((1, 0), (4, 2)), ((1, 1), (2, 2)), ((2, 0), (4, 1)))
NORMALS = ((4, 0), (2, 1), (1, 2))
TWISTS = ((3, 0), (5, 1), (6, 2))
BENDS = (((3, 1), (5, 0)), ((3, 2), (6, 0)), ((5, 2), (6, 1)))


def check_table():
    table = np.zeros((24, 24))

    def put(a, b, v):
        table[3 * a[0] + a[1], 3 * b[0] + b[1]] = v

    for a, b in SHEAR_PAIRS:
        for u in (a, b):
            for v in (a, b):
                put(u, v, SHEAR)
    for a in NORMALS:
        for b in NORMALS:
            put(a, b, TRACE + (NORMAL if a == b else 0))
    for a in TWISTS:
        for b in TWISTS:
            put(a, b, 2 * TWIST if a == b else TWIST)
    for a, b in BENDS:
        put(a, a, BEND)
        put(b, b, BEND)
        put(a, b, CROSS)
        put(b, a, CROSS)
    for c in range(3):
        put((7, c), (7, c), LAST)
    assert np.abs(table - KHAT).max() < 1e-8


check_table()


def shift_rows_up(v, after, row):
    return pltpu.roll(jnp.where(row == 0, after, v), 7, 0)


def plane_modes(v, after, row, col):
    ahead = shift_rows_up(v, after, row)
    out = {}
    for px, f in ((0, v + ahead), (1, ahead - v)):
        fa = jnp.where(col == COLS - 1, 0.0, pltpu.roll(f, COLS - 1, 1))
        out[px, 0] = f + fa
        out[px, 1] = fa - f
    return out


def cell_modes(bottom, top):
    m = {}
    for c in range(3):
        for p in range(1, 8):
            xy = (p >> 1 & 1, p & 1)
            b, t = bottom[c][xy], top[c][xy]
            m[p, c] = t - b if p >> 2 else t + b
    return m


def cell_forces(m, stiff):
    f = {}
    shear, trace, normal = stiff * SHEAR, stiff * TRACE, stiff * NORMAL
    twist, bend, cross, last = stiff * TWIST, stiff * BEND, stiff * CROSS, stiff * LAST
    for a, b in SHEAR_PAIRS:
        f[a] = f[b] = shear * (m[a] + m[b])
    total = trace * (m[NORMALS[0]] + m[NORMALS[1]] + m[NORMALS[2]])
    for a in NORMALS:
        f[a] = total + normal * m[a]
    total = m[TWISTS[0]] + m[TWISTS[1]] + m[TWISTS[2]]
    for a in TWISTS:
        f[a] = twist * (total + m[a])
    for a, b in BENDS:
        f[a] = bend * m[a] + cross * m[b]
        f[b] = cross * m[a] + bend * m[b]
    for c in range(3):
        f[7, c] = last * m[7, c]
    return f


def cell_energy(m):
    shear = None
    for a, b in SHEAR_PAIRS:
        s = m[a] + m[b]
        shear = s * s if shear is None else shear + s * s
    total = m[NORMALS[0]] + m[NORMALS[1]] + m[NORMALS[2]]
    normal = m[NORMALS[0]] * m[NORMALS[0]] + m[NORMALS[1]] * m[NORMALS[1]] + m[NORMALS[2]] * m[NORMALS[2]]
    twist = m[TWISTS[0]] + m[TWISTS[1]] + m[TWISTS[2]]
    twists = twist * twist
    for a in TWISTS:
        twists = twists + m[a] * m[a]
    bends = None
    crosses = None
    for a, b in BENDS:
        s = m[a] * m[a] + m[b] * m[b]
        t = m[a] * m[b]
        bends = s if bends is None else bends + s
        crosses = t if crosses is None else crosses + t
    last = m[7, 0] * m[7, 0] + m[7, 1] * m[7, 1] + m[7, 2] * m[7, 2]
    return (
        SHEAR * shear
        + TRACE * (total * total)
        + NORMAL * normal
        + TWIST * twists
        + BEND * bends
        + (2.0 * CROSS) * crosses
        + LAST * last
    )


def gauss(count):
    t = (
        lax.broadcasted_iota(jnp.int32, (count, count), 0)
        - lax.broadcasted_iota(jnp.int32, (count, count), 1)
    ).astype(F32) * (1.0 / RADIUS)
    return jnp.exp(-(t * t))


def dot(a, b):
    return lax.dot_general(
        a, b, (((1,), (0,)), ((), ())), precision=HIGHEST, preferred_element_type=F32
    )


def total_of(tile):
    return jnp.sum(jnp.sum(tile, axis=0, keepdims=True), axis=1, keepdims=True)


def chebyshev(upper):
    lower = LOWER_RATIO * upper
    center = 0.5 * (upper + lower)
    half_width = 0.5 * (upper - lower)
    spread = center / half_width
    factor = 1.0 / spread
    zero = jnp.zeros_like(upper)
    e = [jnp.ones_like(upper)] + [zero] * (SWEEPS - 1)
    d = [1.0 / center] + [zero] * (SWEEPS - 1)
    u = [zero] * SWEEPS
    for sweep in range(SWEEPS):
        u = [a + b for a, b in zip(u, d)]
        if sweep < SWEEPS - 1:
            e = [e[0]] + [e[n] - d[n - 1] for n in range(1, SWEEPS)]
            after = 1.0 / (2.0 * spread - factor)
            d = [after * factor * a + 2.0 * after / half_width * b for a, b in zip(d, e)]
            factor = after
    return u


def kernel(
    u0_ref, dens_ref, des_ref, sup_ref, nodes_ref, forces_ref,
    disp_out, dens_out,
    t_buf, v_buf, u0_buf, rhs_buf, c_buf, sup_buf, stiff_buf, inv_buf, free_buf,
    tu_buf, send_buf, back_buf, coef_buf, dp_buf,
    fz_buf, ps_buf, fy_buf, smooth_buf, xq_buf, q_buf, num_buf, rs_buf, dt_buf, xt_buf,
    den_buf, sz_buf, sy_buf, wx_buf, wz_buf, wy_buf, vol_buf,
    recv, send, xsend, xrecv, zsend, zrecv, ysend, yrecv, vsend, vrecv,
):
    s = lax.axis_index("slab")
    l = lax.axis_index("load")
    h = lax.rem(s, 2)
    k = s // 2
    z = lax.rem(k, NZ_)
    y = k // NZ_
    j = h * LOADS_AX + l
    other = 1 - h

    def at(group, half=None, load=None):
        return {
            "slab": group * 2 + (h if half is None else half),
            "load": l if load is None else load,
        }

    above = lax.rem(k + 1, PLANE)
    below = lax.rem(k + PLANE - 1, PLANE)
    partner = at(k, half=other)

    def ring_peer(d):
        t = lax.rem(j + d, RING)
        return t, at(k, half=t // LOADS_AX, load=lax.rem(t, LOADS_AX))

    def z_peer(d):
        return at(y * NZ_ + lax.rem(z + d, NZ_))

    def y_peer(d):
        return at(lax.rem(y + d, NY_) * NZ_ + z)

    def plane_peer(dy, dz):
        return at(lax.rem(y + dy, NY_) * NZ_ + lax.rem(z + dz, NZ_))

    barrier = pltpu.get_barrier_semaphore()
    for d in range(1, RING):
        pl.semaphore_signal(barrier, inc=1, device_id=ring_peer(d)[1], device_id_type=MESH)
    for dy in range(NY_):
        for dz in range(NZ_):
            if dy or dz:
                pl.semaphore_signal(
                    barrier, inc=1, device_id=plane_peer(dy, dz), device_id_type=MESH
                )

    waits = []

    def remote(src, dst, ss, rs, device):
        copy = pltpu.make_async_remote_copy(
            src_ref=src, dst_ref=dst, send_sem=ss, recv_sem=rs,
            device_id=device, device_id_type=MESH,
        )
        copy.start()
        waits.append(copy)
        return copy

    row = lax.broadcasted_iota(jnp.int32, (8, COLS), 0)
    col = lax.broadcasted_iota(jnp.int32, (8, COLS), 1)

    dens = dens_ref[0]
    solid = des_ref[0].astype(F32) * dens
    c_buf[1 + h] = solid * solid * solid
    sup_buf[h] = sup_ref[0]
    free_own = 1.0 - sup_ref[0].astype(F32)
    for c in range(3):
        mine = u0_ref[h, c, 0]
        u0_buf[h, c] = mine
        t_buf[0, 1 + h, c, 0:ROWS] = mine * free_own
    zero8 = jnp.zeros((8, COLS), F32)
    for step in range(SWEEPS + 1):
        for n in range(4):
            for c in range(3):
                t_buf[step, n, c, ROWS : ROWS + 8] = zero8
    for n in range(1, 4):
        for c in range(3):
            tu_buf[n, c, ROWS : ROWS + 8] = zero8
    gauss_x, gauss_y = gauss(ROWS), gauss(COLS)
    smooth_buf[...] = dot(dot(gauss_x, dens), gauss_y)
    mine8 = pl.ds(pl.multiple_of(8 * j, 8), 8)
    jp = other * LOADS_AX + l
    other8 = pl.ds(pl.multiple_of(8 * jp, 8), 8)
    fz_buf[0, 0, h] = smooth_buf[mine8]
    dp_buf[h] = dens_ref[0, mine8]

    pl.semaphore_wait(barrier, RING - 1 + PLANE - 1)

    got_u0 = remote(u0_ref.at[other, :, 0], u0_buf.at[h], send.at[0], recv.at[0], partner)
    got_sup = remote(sup_ref.at[0], sup_buf.at[h], send.at[1], recv.at[1], partner)
    got_c = remote(c_buf.at[1 + h], c_buf.at[1 + h], send.at[2], recv.at[2], partner)
    toward = jnp.where(h == 0, below, above)
    away = jnp.where(h == 0, above, below)
    rows64 = pl.ds(0, ROWS)
    got_t1 = remote(
        t_buf.at[0, 1 + h, :, rows64], t_buf.at[0, 3 * other, :, rows64],
        send.at[3], recv.at[3], at(toward),
    )
    got_sm = remote(smooth_buf.at[other8], fz_buf.at[0, 0, h], send.at[4], recv.at[4], partner)
    got_dp = remote(dens_ref.at[0, other8], dp_buf.at[h], send.at[5], recv.at[5], partner)

    base = k * (2 * ROWS)
    wide = (2 * ROWS, CHUNK)
    line = lax.broadcasted_iota(jnp.int32, wide, 0)

    for n in range(2):
        for c in range(3):
            rhs_buf[n, c] = jnp.zeros((ROWS, COLS), F32)

    @pl.loop(0, POINTS // CHUNK)
    def _(i):
        cut = pl.ds(pl.multiple_of(i * CHUNK, CHUNK), CHUNK)
        node = jnp.where(h == 0, nodes_ref[0:1, cut], nodes_ref[1:2, cut])
        place = jnp.where((node >> 7) - base == line, 1.0, 0.0).astype(jnp.bfloat16)
        across = (node & 127) == line
        for c in range(3):
            force = jnp.where(h == 0, forces_ref[0, c : c + 1, cut], forces_ref[1, c : c + 1, cut])
            spread = jnp.where(across, force, 0.0)
            total = jnp.zeros((2 * ROWS, COLS), F32)
            for part in range(3):
                piece = spread.astype(jnp.bfloat16)
                total = total + lax.dot_general(
                    place, piece, (((1,), (1,)), ((), ())), preferred_element_type=F32
                )
                if part < 2:
                    spread = spread - piece.astype(F32)
            rhs_buf[0, c] += total[:ROWS]
            rhs_buf[1, c] += total[ROWS:]

    @pl.loop(0, NY_ * NZ_)
    def _(i):
        dy, dz = i // NZ_, lax.rem(i, NZ_)
        offset = 16 * (lax.rem(y + dy, NY_) - y) + 2 * (z - lax.rem(z + NZ_ - dz, NZ_))
        for a in range(3):
            t = jnp.full((8, COLS), offset + (a - 1), jnp.int32).astype(F32) * (1.0 / RADIUS)
            coef_buf[i * 3 + a] = jnp.exp(-(t * t))

    def z_send(which):
        return [
            remote(
                fz_buf.at[which, 0], fz_buf.at[which, d],
                zsend.at[which, d], zrecv.at[which, d], z_peer(d),
            )
            for d in range(1, NZ_)
        ]

    def z_mix(which, copies):
        for copy in copies:
            copy.wait_recv()

        @pl.loop(0, NY_)
        def _(dy):
            for a in range(2):
                total = None
                for d in range(NZ_):
                    for b in range(2):
                        term = coef_buf[dy * (3 * NZ_) + (3 * d + a - b + 1)] * fz_buf[which, d, b]
                        total = term if total is None else total + term
                ps_buf[which, dy, a] = total

        for a in range(2):
            fy_buf[which, 0, a] = ps_buf[which, 0, a]

    def y_send(which):
        return [
            remote(
                ps_buf.at[which, d], fy_buf.at[which, d],
                ysend.at[which, d], yrecv.at[which, d], y_peer(d),
            )
            for d in range(1, NY_)
        ]

    def y_sum(which, copies):
        for copy in copies:
            copy.wait_recv()
        return [
            fy_buf[which, 0, a] + fy_buf[which, 1, a] + fy_buf[which, 2, a] + fy_buf[which, 3, a]
            for a in range(2)
        ]

    got_c.wait_recv()
    got_up_c = remote(c_buf.at[2], c_buf.at[0], send.at[6], recv.at[6], at(above))
    got_sup.wait_recv()
    got_u0.wait_recv()
    free_other = 1.0 - sup_buf[other].astype(F32)
    for c in range(3):
        t_buf[0, 1 + other, c, 0:ROWS] = u0_buf[other, c] * free_other
    got_t2 = remote(
        t_buf.at[0, 1 + other, :, rows64], t_buf.at[0, 3 * h, :, rows64],
        send.at[7], recv.at[7], at(away),
    )
    for n in range(2):
        free_buf[n] = 1.0 - sup_buf[n].astype(F32)
    got_sm.wait_recv()
    got_dp.wait_recv()
    zs = z_send(0)

    has_below = jnp.where(k > 0, 1.0, 0.0)
    has_above = jnp.where(k < PLANE - 1, 1.0, 0.0)
    got_up_c.wait_recv()
    for e in range(3):
        stiff = STIFF_VOID + (1.0 - STIFF_VOID) * c_buf[e]
        stiff_buf[e] = stiff * has_below if e == 0 else stiff

    @pl.loop(0, ROWS // 8, init_carry=(zero8, zero8))
    def _(i, carry):
        rows = pl.ds(pl.multiple_of(i * 8, 8), 8)
        out = []
        for n in range(2):
            b = stiff_buf[n, rows] + stiff_buf[n + 1, rows]
            b = b + jnp.where(col == 0, 0.0, pltpu.roll(b, 1, 1))
            r = pltpu.roll(b, 1, 0)
            b = b + jnp.where(row == 0, carry[n], r)
            out.append(r)
            free = free_buf[n, rows]
            inv_buf[n, rows] = 1.0 / (free * KD * b + (1.0 - free))
        return tuple(out)

    def operate(step, finish, extra):
        def body(i, carry):
            behind, extra = list(carry[0]), carry[1]
            rows = pl.ds(pl.multiple_of(i * 8, 8), 8)
            after = pl.ds(pl.multiple_of(i * 8 + 8, 8), 8)
            total = [None, None]
            lower = None
            for n in range(4):
                upper = []
                for c in range(3):
                    v, w = t_buf[step, n, c, rows], t_buf[step, n, c, after]
                    if n == 3:
                        v, w = v * has_above, w * has_above
                    upper.append(plane_modes(v, w, row, col))
                if n:
                    e = n - 1
                    f = cell_forces(cell_modes(lower, upper), stiff_buf[e, rows])
                    for node, sign in ((e, 1.0), (e - 1, -1.0)):
                        if not 0 <= node < 2:
                            continue
                        part = {}
                        for c in range(3):
                            for q in range(4):
                                hi = f[4 + q, c]
                                if q == 0:
                                    value = hi if sign > 0 else -hi
                                else:
                                    value = f[q, c] + hi if sign > 0 else f[q, c] - hi
                                part[c, q] = value
                        if total[node] is None:
                            total[node] = part
                        else:
                            total[node] = {key: total[node][key] + part[key] for key in part}
                lower = upper
            for node in range(2):
                for c in range(3):
                    g = []
                    for px in range(2):
                        fs, fd = total[node][c, 2 * px], total[node][c, 2 * px + 1]
                        shifted = jnp.where(col == 0, 0.0, pltpu.roll(fs + fd, 1, 1))
                        g.append(fs - fd + shifted)
                    r = pltpu.roll(g[0] + g[1], 1, 0)
                    slot = 3 * node + c
                    value = g[0] - g[1] + jnp.where(row == 0, behind[slot], r)
                    behind[slot] = r
                    extra = finish(node, c, rows, value, extra)
            return tuple(behind), extra

        return lax.fori_loop(0, ROWS // 8, body, ((zero8,) * 6, extra))[1]

    def send_layers(step):
        up = remote(
            t_buf.at[step, 2, :, rows64], t_buf.at[step, 0, :, rows64],
            send.at[6 + 2 * step], recv.at[6 + 2 * step], at(above),
        )
        down = remote(
            t_buf.at[step, 1, :, rows64], t_buf.at[step, 3, :, rows64],
            send.at[7 + 2 * step], recv.at[7 + 2 * step], at(below),
        )
        return up, down

    def wait_layers(copies):
        for copy in copies:
            copy.wait_recv()

    def first(n, c, rows, value, extra):
        free, inv = free_buf[n, rows], inv_buf[n, rows]
        r = free * (rhs_buf[n, c, rows] - value) - (1.0 - free) * u0_buf[n, c, rows]
        g = r * inv
        v_buf[0, n, c, rows] = g
        t_buf[1, 1 + n, c, rows] = free * g
        return extra + r * g

    def later(step):
        def finish(n, c, rows, value, extra):
            free, inv = free_buf[n, rows], inv_buf[n, rows]
            v = v_buf[step - 1, n, c, rows]
            w = free * value + (1.0 - free) * v
            new = w * inv
            v_buf[step, n, c, rows] = new
            t_buf[step + 1, 1 + n, c, rows] = free * new
            return extra + v * w if step == 1 else extra

        return finish

    wait_layers((got_t1, got_t2))
    gr = operate(0, first, zero8)
    flight = send_layers(1)
    z_mix(0, zs)
    ys = y_send(0)
    wait_layers(flight)
    gw = operate(1, later(1), zero8)
    flight = send_layers(2)

    count8 = jnp.zeros((8, COLS), F32)
    for n in range(2):
        for i in range(ROWS // 8):
            count8 = count8 + jnp.where(c_buf[1 + n, 8 * i : 8 * i + 8] > 0.0, 1.0, 0.0)
    sums = [jnp.sum(t, axis=0, keepdims=True) for t in (gr, gw, count8)]
    tile = jnp.where(row == 0, sums[0], jnp.where(row == 1, sums[1], jnp.where(row == 2, sums[2], 0.0)))
    sz_buf[0] = tile
    scalar_z = [
        remote(sz_buf.at[0], sz_buf.at[d], zsend.at[3, d], zrecv.at[3, d], z_peer(d))
        for d in range(1, NZ_)
    ]
    denom = y_sum(0, ys)
    design_here = []
    for a in range(2):
        den_buf[a] = denom[a]
        fz_buf[1, 0, a] = jnp.where(c_buf[1 + a, mine8] > 0.0, 1.0, 0.0) / denom[a]
    zs = z_send(1)
    wait_layers(flight)
    operate(2, later(2), 0)
    flight = send_layers(3)
    for copy in scalar_z:
        copy.wait_recv()
    tile = sz_buf[0]
    for d in range(1, NZ_):
        tile = tile + sz_buf[d]
    sy_buf[0] = tile
    scalar_y = [
        remote(sy_buf.at[0], sy_buf.at[d], ysend.at[3, d], yrecv.at[3, d], y_peer(d))
        for d in range(1, NY_)
    ]
    z_mix(1, zs)
    ys = y_send(1)
    wait_layers(flight)
    operate(3, later(3), 0)
    got_last = remote(
        t_buf.at[4, 1, :, rows64], t_buf.at[4, 3, :, rows64],
        send.at[14], recv.at[14], at(below),
    )
    for copy in scalar_y:
        copy.wait_recv()
    tile = sy_buf[0] + sy_buf[1] + sy_buf[2] + sy_buf[3]
    gr_all = jnp.sum(tile[0:1], axis=1, keepdims=True)
    gw_all = jnp.sum(tile[1:2], axis=1, keepdims=True)
    count = jnp.sum(tile[2:3], axis=1, keepdims=True)
    coefs = [jnp.broadcast_to(c, (8, COLS)) for c in chebyshev(UPPER_FACTOR * gw_all / gr_all)]

    @pl.loop(0, ROWS // 8)
    def _(i):
        rows = pl.ds(pl.multiple_of(i * 8, 8), 8)
        for n in range(2):
            free = free_buf[n, rows]
            for c in range(3):
                u = u0_buf[n, c, rows]
                for power in range(SWEEPS):
                    u = u + coefs[power] * v_buf[power, n, c, rows]
                send_buf[n, c, rows] = u
                tu_buf[1 + n, c, rows] = free * u

    got_back = remote(send_buf.at[other], back_buf, send.at[15], recv.at[15], partner)
    for c in range(3):
        disp_out[h, c, 0] = send_buf[h, c]

    q8 = y_sum(1, ys)
    for a in range(2):
        xq_buf[0, a] = q8[a]

    def ring_send(which, src, dst):
        out = []
        for d in range(1, RING):
            t, device = ring_peer(d)
            out.append(remote(src(t), dst(d), xsend.at[which, d], xrecv.at[which, d], device))
        return out

    xs = ring_send(0, lambda t: xq_buf.at[0], lambda d: xq_buf.at[d])

    def energy(e):
        @pl.loop(0, ROWS // 8)
        def _(i):
            rows = pl.ds(pl.multiple_of(i * 8, 8), 8)
            after = pl.ds(pl.multiple_of(i * 8 + 8, 8), 8)
            planes = [
                [plane_modes(tu_buf[n, c, rows], tu_buf[n, c, after], row, col) for c in range(3)]
                for n in (e, e + 1)
            ]
            value = cell_energy(cell_modes(*planes))
            weight = (3.0 * (1.0 - STIFF_VOID)) * c_buf[e, rows]
            num_buf[e - 1, rows] = weight * value

    def smooth_xy(read):
        mixed = dot(jnp.concatenate([read(0), read(1)], 0), gauss_y)
        return [dot(gauss_x, mixed[ROWS * a : ROWS * a + ROWS]) for a in range(2)]

    energy(1)
    for copy in xs:
        copy.wait_recv()
    for d in range(RING):
        there = pl.ds(pl.multiple_of(8 * lax.rem(j + RING - d, RING), 8), 8)
        for a in range(2):
            q_buf[a, there] = xq_buf[d, a]
    q = smooth_xy(lambda a: q_buf[a])
    for a in range(2):
        q_buf[a] = q[a]

    got_last.wait_recv()

    @pl.loop(0, ROWS // 8)
    def _(i):
        rows = pl.ds(pl.multiple_of(i * 8, 8), 8)
        for c in range(3):
            u = t_buf[0, 3, c, rows]
            for power in range(SWEEPS):
                u = u + coefs[power] * t_buf[power + 1, 3, c, rows]
            tu_buf[3, c, rows] = u * has_above

    energy(2)
    part = jnp.zeros((8, COLS), F32)
    for a in range(2):
        for i in range(ROWS // 8):
            cut = slice(8 * i, 8 * i + 8)
            part = part + q_buf[a, cut] * num_buf[a, cut]
    wx_buf[0] = part
    wxs = ring_send(1, lambda t: wx_buf.at[0], lambda d: wx_buf.at[d])
    numer = smooth_xy(lambda a: num_buf[a])
    for a in range(2):
        num_buf[a] = numer[a]
    for a in range(2):
        rs_buf[0, a] = num_buf[a, mine8]
    xs = ring_send(
        2,
        lambda t: num_buf.at[:, pl.ds(pl.multiple_of(8 * t, 8), 8)],
        lambda d: rs_buf.at[d],
    )
    for copy in wxs:
        copy.wait_recv()
    tile = wx_buf[0]
    for d in range(1, RING):
        tile = tile + wx_buf[d]
    wz_buf[0] = tile
    wzs = [
        remote(wz_buf.at[0], wz_buf.at[d], zsend.at[4, d], zrecv.at[4, d], z_peer(d))
        for d in range(1, NZ_)
    ]
    for copy in xs:
        copy.wait_recv()
    for a in range(2):
        total = rs_buf[0, a]
        for d in range(1, RING):
            total = total + rs_buf[d, a]
        fz_buf[2, 0, a] = total
    zs = z_send(2)
    for copy in wzs:
        copy.wait_recv()
    tile = wz_buf[0]
    for d in range(1, NZ_):
        tile = tile + wz_buf[d]
    wy_buf[0] = tile
    wys = [
        remote(wy_buf.at[0], wy_buf.at[d], ysend.at[4, d], yrecv.at[4, d], y_peer(d))
        for d in range(1, NY_)
    ]
    z_mix(2, zs)
    ys = y_send(2)
    for copy in wys:
        copy.wait_recv()
    weighted_all = total_of(wy_buf[0] + wy_buf[1] + wy_buf[2] + wy_buf[3])
    inv_mean = 1.0 / (weighted_all / count + EPSILON)
    numer = y_sum(2, ys)
    for a in range(2):
        here = jnp.where(c_buf[1 + a, mine8] > 0.0, 1.0, 0.0)
        weighted = here * (numer[a] / den_buf[a])
        ratio = weighted * inv_mean
        old = dp_buf[a]
        trial = jnp.minimum(
            jnp.maximum(old * jnp.sqrt(ratio), old - MOVE_LIMIT), old + MOVE_LIMIT
        )
        xt_buf[0, a] = here * trial
    xs = ring_send(3, lambda t: xt_buf.at[0], lambda d: xt_buf.at[d])
    for copy in xs:
        copy.wait_recv()
    tile = None
    for d in range(RING):
        for a in range(2):
            tile = xt_buf[d, a] if tile is None else tile + xt_buf[d, a]
    vol_buf[0] = jnp.sum(tile, axis=0, keepdims=True)
    vs = [
        remote(
            vol_buf.at[0], vol_buf.at[dy * NZ_ + dz],
            vsend.at[dy * NZ_ + dz], vrecv.at[dy * NZ_ + dz], plane_peer(dy, dz),
        )
        for dy in range(NY_)
        for dz in range(NZ_)
        if dy or dz
    ]
    got_back.wait_recv()
    for c in range(3):
        disp_out[other, c, 0] = back_buf[c]
    for copy in vs:
        copy.wait_recv()
    tile = vol_buf[0]
    for i in range(1, PLANE):
        tile = tile + vol_buf[i]
    volume = jnp.sum(tile, axis=1, keepdims=True)
    scale = VOLUME_TARGET / (volume / count + EPSILON)
    for d in range(RING):
        there = pl.ds(pl.multiple_of(8 * lax.rem(j + RING - d, RING), 8), 8)
        dens_out[0, there] = jnp.minimum(scale * xt_buf[d, h], 1.0)
    for copy in waits:
        copy.wait_send()


def shards(start_disp, density, design, support, load_nodes, load_forces):
    vmem = lambda *shape: pltpu.VMEM(shape, F32)
    dma = lambda *shape: pltpu.SemaphoreType.DMA(shape)
    plane = (ROWS, COLS)
    return pl.pallas_call(
        kernel,
        out_shape=(
            jax.ShapeDtypeStruct(start_disp.shape, F32),
            jax.ShapeDtypeStruct(density.shape, F32),
        ),
        in_specs=[pl.BlockSpec(memory_space=pltpu.VMEM)] * 6,
        out_specs=(pl.BlockSpec(memory_space=pltpu.VMEM),) * 2,
        scratch_shapes=[
            vmem(SWEEPS + 1, 4, 3, ROWS + 8, COLS),
            vmem(SWEEPS, 2, 3, *plane),
            vmem(2, 3, *plane),
            vmem(2, 3, *plane),
            vmem(3, *plane),
            pltpu.VMEM((2, *plane), jnp.int32),
            vmem(3, *plane),
            vmem(2, *plane),
            vmem(2, *plane),
            vmem(4, 3, ROWS + 8, COLS),
            vmem(2, 3, *plane),
            vmem(3, *plane),
            vmem(3 * NY_ * NZ_, 8, COLS),
            vmem(2, 8, COLS),
            vmem(3, NZ_, 2, 8, COLS),
            vmem(3, NY_, 2, 8, COLS),
            vmem(3, NY_, 2, 8, COLS),
            vmem(*plane),
            vmem(RING, 2, 8, COLS),
            vmem(2, *plane),
            vmem(2, *plane),
            vmem(RING, 2, 8, COLS),
            vmem(2, 8, COLS),
            vmem(RING, 2, 8, COLS),
            vmem(2, 8, COLS),
            vmem(NZ_, 8, COLS),
            vmem(NY_, 8, COLS),
            vmem(RING, 8, COLS),
            vmem(NZ_, 8, COLS),
            vmem(NY_, 8, COLS),
            vmem(PLANE, 1, COLS),
            dma(16), dma(16),
            dma(4, RING), dma(4, RING),
            dma(5, NZ_), dma(5, NZ_),
            dma(5, NY_), dma(5, NY_),
            dma(PLANE), dma(PLANE),
        ],
        compiler_params=pltpu.CompilerParams(
            collective_id=0, has_side_effects=True, vmem_limit_bytes=48 * 1024 * 1024
        ),
    )(start_disp, density, design, support, load_nodes, load_forces)


def solution(mesh):
    return jax.shard_map(
        shards,
        mesh=mesh,
        in_specs=(
            P("load", None, "slab", None, None),
            P("slab", None, None),
            P("slab", None, None),
            P("slab", None, None),
            P("load", None),
            P("load", None, None),
        ),
        out_specs=(P("load", None, "slab", None, None), P("slab", None, None)),
        check_vma=False,
    )
```

```python
import contextlib

import jax
import jax.numpy as jnp
import numpy as np
from jax import lax
from jax.experimental import pallas as pl
from jax.experimental.pallas import tpu as pltpu
from jax.sharding import PartitionSpec as P

SWEEPS = 4
RADIUS = 2
POISSON = 0.3
STIFF_VOID = 0.001
UPPER_FACTOR = 1.2
LOWER_RATIO = 0.1
MOVE_LIMIT = 0.2
VOLUME_TARGET = 0.5
EPSILON = 1e-06
HIGHEST = lax.Precision.HIGHEST
MESH = pl.DeviceIdType.MESH
F32 = jnp.float32

NY_, NZ_ = 4, 8
LOADS_AX = 4
RING = 2 * LOADS_AX
PLANE = NY_ * NZ_
ROWS, COLS = 64, 128
POINTS = 2048
CHUNK = 256
PIECE = 16
PIECES = ROWS // PIECE


def hex_stiffness():
    lame_first = POISSON / ((1 + POISSON) * (1 - 2 * POISSON))
    lame_shear = 1 / (2 * (1 + POISSON))
    elastic = np.zeros((6, 6))
    elastic[:3, :3] = lame_first
    for axis_a in range(3):
        elastic[axis_a, axis_a] += 2 * lame_shear
        elastic[3 + axis_a, 3 + axis_a] = lame_shear
    shear_pairs = ((0, 1), (1, 2), (0, 2))
    gauss_point = 1 / np.sqrt(3)
    matrix = np.zeros((24, 24))
    for quad_index in range(8):
        quad_coords = [
            gauss_point * (2 * (quad_index >> 2 - axis_a & 1) - 1) for axis_a in range(3)
        ]
        shape_grads = np.zeros((8, 3))
        for corner in range(8):
            corner_signs = [2 * (corner >> 2 - axis_a & 1) - 1 for axis_a in range(3)]
            for axis_a in range(3):
                deriv_value = float(corner_signs[axis_a])
                for axis_b in range(3):
                    if axis_b != axis_a:
                        deriv_value *= (1 + corner_signs[axis_b] * quad_coords[axis_b]) / 2
                shape_grads[corner, axis_a] = deriv_value
        strain = np.zeros((6, 24))
        for corner in range(8):
            for axis_a in range(3):
                strain[axis_a, 3 * corner + axis_a] = shape_grads[corner, axis_a]
            for pair_index, shear_pair in enumerate(shear_pairs):
                strain[3 + pair_index, 3 * corner + shear_pair[0]] = shape_grads[
                    corner, shear_pair[1]
                ]
                strain[3 + pair_index, 3 * corner + shear_pair[1]] = shape_grads[
                    corner, shear_pair[0]
                ]
        matrix += strain.T @ elastic @ strain / 8
    return matrix.astype(np.float32)


def mode_stiffness():
    ke = hex_stiffness().astype(np.float64)
    w = np.zeros((24, 24))
    for p in range(8):
        for o in range(8):
            sign = 1.0
            for a in range(3):
                if p >> (2 - a) & 1:
                    sign *= 1.0 if o >> (2 - a) & 1 else -1.0
            for c in range(3):
                w[3 * p + c, 3 * o + c] = sign
    return w @ ke @ w.T / 64


KHAT = mode_stiffness()
KD = float(hex_stiffness()[0, 0])


def kh(p, c, q, d):
    return float(KHAT[3 * p + c, 3 * q + d])


SHEAR = kh(1, 0, 1, 0)
TRACE = kh(1, 2, 2, 1)
NORMAL = kh(1, 2, 1, 2) - TRACE
TWIST = kh(3, 0, 5, 1)
BEND = kh(3, 1, 3, 1)
CROSS = kh(3, 1, 5, 0)
LAST = kh(7, 0, 7, 0)

SHEAR_PAIRS = (((1, 0), (4, 2)), ((1, 1), (2, 2)), ((2, 0), (4, 1)))
NORMALS = ((4, 0), (2, 1), (1, 2))
TWISTS = ((3, 0), (5, 1), (6, 2))
BENDS = (((3, 1), (5, 0)), ((3, 2), (6, 0)), ((5, 2), (6, 1)))


def check_table():
    table = np.zeros((24, 24))

    def put(a, b, v):
        table[3 * a[0] + a[1], 3 * b[0] + b[1]] = v

    for a, b in SHEAR_PAIRS:
        for u in (a, b):
            for v in (a, b):
                put(u, v, SHEAR)
    for a in NORMALS:
        for b in NORMALS:
            put(a, b, TRACE + (NORMAL if a == b else 0))
    for a in TWISTS:
        for b in TWISTS:
            put(a, b, 2 * TWIST if a == b else TWIST)
    for a, b in BENDS:
        put(a, a, BEND)
        put(b, b, BEND)
        put(a, b, CROSS)
        put(b, a, CROSS)
    for c in range(3):
        put((7, c), (7, c), LAST)
    assert np.abs(table - KHAT).max() < 1e-8


check_table()


def shift_rows_up(v, after, row):
    return pltpu.roll(jnp.where(row == 0, after, v), 7, 0)


def plane_modes(v, after, row, col):
    ahead = shift_rows_up(v, after, row)
    out = {}
    for px, f in ((0, v + ahead), (1, ahead - v)):
        fa = jnp.where(col == COLS - 1, 0.0, pltpu.roll(f, COLS - 1, 1))
        out[px, 0] = f + fa
        out[px, 1] = fa - f
    return out


def cell_modes(bottom, top):
    m = {}
    for c in range(3):
        for p in range(1, 8):
            xy = (p >> 1 & 1, p & 1)
            b, t = bottom[c][xy], top[c][xy]
            m[p, c] = t - b if p >> 2 else t + b
    return m


def cell_forces(m, stiff):
    f = {}
    shear, trace, normal = stiff * SHEAR, stiff * TRACE, stiff * NORMAL
    twist, bend, cross, last = stiff * TWIST, stiff * BEND, stiff * CROSS, stiff * LAST
    for a, b in SHEAR_PAIRS:
        f[a] = f[b] = shear * (m[a] + m[b])
    total = trace * (m[NORMALS[0]] + m[NORMALS[1]] + m[NORMALS[2]])
    for a in NORMALS:
        f[a] = total + normal * m[a]
    total = m[TWISTS[0]] + m[TWISTS[1]] + m[TWISTS[2]]
    for a in TWISTS:
        f[a] = twist * (total + m[a])
    for a, b in BENDS:
        f[a] = bend * m[a] + cross * m[b]
        f[b] = cross * m[a] + bend * m[b]
    for c in range(3):
        f[7, c] = last * m[7, c]
    return f


def cell_energy(m):
    shear = None
    for a, b in SHEAR_PAIRS:
        s = m[a] + m[b]
        shear = s * s if shear is None else shear + s * s
    total = m[NORMALS[0]] + m[NORMALS[1]] + m[NORMALS[2]]
    normal = m[NORMALS[0]] * m[NORMALS[0]] + m[NORMALS[1]] * m[NORMALS[1]] + m[NORMALS[2]] * m[NORMALS[2]]
    twist = m[TWISTS[0]] + m[TWISTS[1]] + m[TWISTS[2]]
    twists = twist * twist
    for a in TWISTS:
        twists = twists + m[a] * m[a]
    bends = None
    crosses = None
    for a, b in BENDS:
        s = m[a] * m[a] + m[b] * m[b]
        t = m[a] * m[b]
        bends = s if bends is None else bends + s
        crosses = t if crosses is None else crosses + t
    last = m[7, 0] * m[7, 0] + m[7, 1] * m[7, 1] + m[7, 2] * m[7, 2]
    return (
        SHEAR * shear
        + TRACE * (total * total)
        + NORMAL * normal
        + TWIST * twists
        + BEND * bends
        + (2.0 * CROSS) * crosses
        + LAST * last
    )


def gauss(count):
    t = (
        lax.broadcasted_iota(jnp.int32, (count, count), 0)
        - lax.broadcasted_iota(jnp.int32, (count, count), 1)
    ).astype(F32) * (1.0 / RADIUS)
    return jnp.exp(-(t * t))


def dot(a, b):
    return lax.dot_general(
        a, b, (((1,), (0,)), ((), ())), precision=HIGHEST, preferred_element_type=F32
    )


def total_of(tile):
    return jnp.sum(jnp.sum(tile, axis=0, keepdims=True), axis=1, keepdims=True)


def chebyshev(upper):
    lower = LOWER_RATIO * upper
    center = 0.5 * (upper + lower)
    half_width = 0.5 * (upper - lower)
    spread = center / half_width
    factor = 1.0 / spread
    zero = jnp.zeros_like(upper)
    e = [jnp.ones_like(upper)] + [zero] * (SWEEPS - 1)
    d = [1.0 / center] + [zero] * (SWEEPS - 1)
    u = [zero] * SWEEPS
    for sweep in range(SWEEPS):
        u = [a + b for a, b in zip(u, d)]
        if sweep < SWEEPS - 1:
            e = [e[0]] + [e[n] - d[n - 1] for n in range(1, SWEEPS)]
            after = 1.0 / (2.0 * spread - factor)
            d = [after * factor * a + 2.0 * after / half_width * b for a, b in zip(d, e)]
            factor = after
    return u


def kernel(
    u0_ref, dens_ref, des_ref, sup_ref, nodes_ref, forces_ref,
    disp_out, dens_out,
    t_buf, v_buf, u0_buf, rhs_buf, c_buf, stiff_buf, inv_buf, free_buf,
    swap_out, swap_in, tu_buf, send_buf, back_buf, coef_buf, row_out, row_in,
    fz_buf, ps_buf, fy_buf, smooth_buf, xq_buf, q_buf, num_buf, rs_buf, xt_buf,
    den_buf, sz_buf, sy_buf, wx_buf, wz_buf, wy_buf, vol_buf,
    swap_recv, halo_recv, c_recv, halo_send, one_send, one_recv, group_send, group_recv,
):
    s = lax.axis_index("slab")
    l = lax.axis_index("load")
    h = lax.rem(s, 2)
    k = s // 2
    z = lax.rem(k, NZ_)
    y = k // NZ_
    j = h * LOADS_AX + l
    other = 1 - h

    def at(group, half=None, load=None):
        return {
            "slab": group * 2 + (h if half is None else half),
            "load": l if load is None else load,
        }

    above = lax.rem(k + 1, PLANE)
    below = lax.rem(k + PLANE - 1, PLANE)
    partner = at(k, half=other)

    def ring_peer(d):
        t = lax.rem(j + d, RING)
        return t, at(k, half=t // LOADS_AX, load=lax.rem(t, LOADS_AX))

    def z_peer(d):
        return at(y * NZ_ + lax.rem(z + d, NZ_))

    def y_peer(d):
        return at(lax.rem(y + d, NY_) * NZ_ + z)

    def plane_peer(i):
        return at(lax.rem(y + i // NZ_, NY_) * NZ_ + lax.rem(z + i % NZ_, NZ_))

    phases = contextlib.ExitStack()

    def mark(name):
        phases.close()
        if name:
            phases.enter_context(jax.named_scope(name))

    mark("signals")
    barrier = pltpu.get_barrier_semaphore()
    for d in range(1, RING):
        pl.semaphore_signal(barrier, inc=1, device_id=ring_peer(d)[1], device_id_type=MESH)
    for i in range(1, PLANE):
        pl.semaphore_signal(barrier, inc=1, device_id=plane_peer(i), device_id_type=MESH)

    sent = []

    def start(src, dst, ss, rs, device):
        copy = pltpu.make_async_remote_copy(
            src_ref=src, dst_ref=dst, send_sem=ss, recv_sem=rs,
            device_id=device, device_id_type=MESH,
        )
        copy.start()
        return copy

    def whole(ref, ss, rs):
        return pltpu.make_async_remote_copy(
            src_ref=ref, dst_ref=ref, send_sem=ss, recv_sem=rs,
            device_id=partner, device_id_type=MESH,
        )

    def one(slot, src, dst, device):
        copy = start(src, dst, one_send.at[slot], one_recv.at[slot], device)
        sent.append(copy)
        return copy

    def group(slot, buf, count, src, peer):
        for d in range(1, count):
            start(src(d), buf.at[d], group_send.at[slot], group_recv.at[slot], peer(d))
        rest = whole(buf.at[pl.ds(1, count - 1)], group_send.at[slot], group_recv.at[slot])
        sent.append(rest)
        return rest

    row = lax.broadcasted_iota(jnp.int32, (8, COLS), 0)
    col = lax.broadcasted_iota(jnp.int32, (8, COLS), 1)
    zero8 = jnp.zeros((8, COLS), F32)

    mark("prep")
    dens = dens_ref[0]
    solid = des_ref[0].astype(F32) * dens
    cube = solid * solid * solid
    free_own = 1.0 - sup_ref[0].astype(F32)
    c_buf[1 + h] = cube
    free_buf[h] = free_own
    swap_out[0] = cube
    swap_out[1] = free_own
    for c in range(3):
        swap_out[2 + c] = u0_ref[other, c, 0]
        mine = u0_ref[h, c, 0]
        u0_buf[h, c] = mine
        t_buf[0, 1 + h, c, 0:ROWS] = mine * free_own
    for step in range(SWEEPS + 1):
        for n in range(4):
            for c in range(3):
                t_buf[step, n, c, ROWS : ROWS + 8] = zero8
    for n in range(2):
        for c in range(3):
            tu_buf[n, c, ROWS : ROWS + 8] = zero8
    gauss_x, gauss_y = gauss(ROWS), gauss(COLS)
    smooth_buf[...] = dot(dot(gauss_x, dens), gauss_y)
    mine8 = pl.ds(pl.multiple_of(8 * j, 8), 8)
    other8 = pl.ds(pl.multiple_of(8 * (other * LOADS_AX + l), 8), 8)
    fz_buf[0, 0, h] = smooth_buf[mine8]
    row_out[0] = smooth_buf[other8]
    row_out[1] = dens_ref[0, other8]

    @pl.loop(0, NY_ * NZ_)
    def _(i):
        dy, dz = i // NZ_, lax.rem(i, NZ_)
        offset = 16 * (lax.rem(y + dy, NY_) - y) + 2 * (z - lax.rem(z + NZ_ - dz, NZ_))
        for a in range(3):
            t = jnp.full((8, COLS), offset + (a - 1), jnp.int32).astype(F32) * (1.0 / RADIUS)
            coef_buf[i * 3 + a] = jnp.exp(-(t * t))

    mark("barrier")
    pl.semaphore_wait(barrier, RING - 1 + PLANE - 1)

    mark("sends0")
    toward = jnp.where(h == 0, below, above)
    away = jnp.where(h == 0, above, below)

    def piece(p):
        if isinstance(p, int):
            return pl.ds(p * PIECE, PIECE)
        return pl.ds(pl.multiple_of(p * PIECE, PIECE), PIECE)

    for p in range(PIECES):
        start(
            swap_out.at[:, piece(p)], swap_in.at[:, piece(p)],
            one_send.at[0], swap_recv.at[p], partner,
        )
    sent.append(whole(swap_out, one_send.at[0], swap_recv.at[0]))
    for p in range(PIECES):
        start(
            t_buf.at[0, 1 + h, :, piece(p)], t_buf.at[0, 3 * other, :, piece(p)],
            halo_send.at[0], halo_recv.at[0, p], at(toward),
        )
    got_rows = one(1, row_out, row_in, partner)

    mark("rhs")
    base = k * (2 * ROWS)
    line = lax.broadcasted_iota(jnp.int32, (2 * ROWS, CHUNK), 0)
    for n in range(2):
        for c in range(3):
            rhs_buf[n, c] = jnp.zeros((ROWS, COLS), F32)

    @pl.loop(0, POINTS // CHUNK)
    def _(i):
        cut = pl.ds(pl.multiple_of(i * CHUNK, CHUNK), CHUNK)
        node = jnp.where(h == 0, nodes_ref[0:1, cut], nodes_ref[1:2, cut])
        place = jnp.where((node >> 7) - base == line, 1.0, 0.0).astype(jnp.bfloat16)
        across = (node & 127) == line
        for c in range(3):
            force = jnp.where(h == 0, forces_ref[c, 0:1, cut], forces_ref[c, 1:2, cut])
            spread = jnp.where(across, force, 0.0)
            total = jnp.zeros((2 * ROWS, COLS), F32)
            for part in range(3):
                bits = spread.astype(jnp.bfloat16)
                total = total + lax.dot_general(
                    place, bits, (((1,), (1,)), ((), ())), preferred_element_type=F32
                )
                if part < 2:
                    spread = spread - bits.astype(F32)
            rhs_buf[0, c] += total[:ROWS]
            rhs_buf[1, c] += total[ROWS:]

    def z_send(slot, which):
        return group(slot, fz_buf.at[which], NZ_, lambda d: fz_buf.at[which, 0], z_peer)

    def z_mix(which):
        @pl.loop(0, NY_)
        def _(dy):
            for a in range(2):
                total = None
                for d in range(NZ_):
                    for b in range(2):
                        term = coef_buf[dy * (3 * NZ_) + (3 * d + a - b + 1)] * fz_buf[which, d, b]
                        total = term if total is None else total + term
                ps_buf[which, dy, a] = total

        for a in range(2):
            fy_buf[which, 0, a] = ps_buf[which, 0, a]

    def y_send(slot, which):
        return group(slot, fy_buf.at[which], NY_, lambda d: ps_buf.at[which, d], y_peer)

    def y_sum(which):
        return [
            fy_buf[which, 0, a] + fy_buf[which, 1, a] + fy_buf[which, 2, a] + fy_buf[which, 3, a]
            for a in range(2)
        ]

    def sum_of(buf, count):
        tile = buf[0]
        for d in range(1, count):
            tile = tile + buf[d]
        return tile

    mark("forward")

    @pl.loop(0, PIECES)
    def _(p):
        rows = piece(p)
        whole(swap_in.at[:, rows], one_send.at[0], swap_recv.at[p]).wait_recv()
        free = swap_in[1, rows]
        free_buf[other, rows] = free
        c_buf[1 + other, rows] = swap_in[0, rows]
        for c in range(3):
            u = swap_in[2 + c, rows]
            u0_buf[other, c, rows] = u
            t_buf[0, 1 + other, c, rows] = u * free
        start(c_buf.at[2, rows], c_buf.at[0, rows], one_send.at[2], c_recv.at[p], at(above))
        start(
            t_buf.at[0, 1 + other, :, rows], t_buf.at[0, 3 * h, :, rows],
            halo_send.at[0], halo_recv.at[0, p], at(away),
        )

    sent.append(whole(c_buf.at[0], one_send.at[2], c_recv.at[0]))
    sent.append(whole(t_buf.at[0, 1:3, :, 0:ROWS], halo_send.at[0], halo_recv.at[0, 0]))
    got_rows.wait_recv()
    fz_buf[0, 0, other] = row_in[0]
    zs = z_send(0, 0)

    has_below = jnp.where(k > 0, 1.0, 0.0)
    has_above = jnp.where(k < PLANE - 1, 1.0, 0.0)

    def wait_piece(step, p):
        if step == 0:
            whole(c_buf.at[0, piece(p)], one_send.at[2], c_recv.at[p]).wait_recv()
        whole(
            t_buf.at[step, 1:3, :, piece(p)], halo_send.at[step], halo_recv.at[step, p]
        ).wait_recv()

    def operate(step, before, finish, extra):
        def chunk(i, behind, extra):
            behind = list(behind)
            rows = pl.ds(pl.multiple_of(i * 8, 8), 8)
            after = pl.ds(pl.multiple_of(i * 8 + 8, 8), 8)
            stiff, extra = before(rows, extra)
            total = [None, None]
            lower = None
            for n in range(4):
                upper = []
                for c in range(3):
                    v, w = t_buf[step, n, c, rows], t_buf[step, n, c, after]
                    if n == 3:
                        v, w = v * has_above, w * has_above
                    upper.append(plane_modes(v, w, row, col))
                if n:
                    e = n - 1
                    f = cell_forces(cell_modes(lower, upper), stiff[e])
                    for node, sign in ((e, 1.0), (e - 1, -1.0)):
                        if not 0 <= node < 2:
                            continue
                        part = {}
                        for c in range(3):
                            for q in range(4):
                                hi = f[4 + q, c]
                                if q == 0:
                                    value = hi if sign > 0 else -hi
                                else:
                                    value = f[q, c] + hi if sign > 0 else f[q, c] - hi
                                part[c, q] = value
                        if total[node] is None:
                            total[node] = part
                        else:
                            total[node] = {key: total[node][key] + part[key] for key in part}
                lower = upper
            for node in range(2):
                for c in range(3):
                    g = []
                    for px in range(2):
                        fs, fd = total[node][c, 2 * px], total[node][c, 2 * px + 1]
                        shifted = jnp.where(col == 0, 0.0, pltpu.roll(fs + fd, 1, 1))
                        g.append(fs - fd + shifted)
                    r = pltpu.roll(g[0] + g[1], 1, 0)
                    slot = 3 * node + c
                    value = g[0] - g[1] + jnp.where(row == 0, behind[slot], r)
                    behind[slot] = r
                    extra = finish(node, c, rows, value, extra)
            return tuple(behind), extra

        def body(p, carry):
            behind, extra = carry

            @pl.when(p < PIECES - 1)
            def _():
                wait_piece(step, p + 1)

            for part in range(PIECE // 8):
                behind, extra = chunk(p * (PIECE // 8) + part, behind, extra)
            send_piece(step + 1, p)
            return behind, extra

        mark(f"wait{step}")
        wait_piece(step, 0)
        mark(f"app{step}")
        out = lax.fori_loop(0, PIECES, body, ((zero8,) * 6, extra))[1]
        return out

    def send_piece(step, p):
        rows = piece(p)
        if step < SWEEPS:
            start(
                t_buf.at[step, 2, :, rows], t_buf.at[step, 0, :, rows],
                halo_send.at[step], halo_recv.at[step, p], at(above),
            )
        start(
            t_buf.at[step, 1, :, rows], t_buf.at[step, 3, :, rows],
            halo_send.at[step], halo_recv.at[step, p], at(below),
        )

    def stiffness(rows, extra):
        acc, rolls = extra
        stiff = [STIFF_VOID + (1.0 - STIFF_VOID) * c_buf[e, rows] for e in range(3)]
        stiff[0] = stiff[0] * has_below
        out = []
        for e in range(3):
            stiff_buf[e, rows] = stiff[e]
        for n in range(2):
            b = stiff[n] + stiff[n + 1]
            b = b + jnp.where(col == 0, 0.0, pltpu.roll(b, 1, 1))
            r = pltpu.roll(b, 1, 0)
            b = b + jnp.where(row == 0, rolls[n], r)
            out.append(r)
            free = free_buf[n, rows]
            inv_buf[n, rows] = 1.0 / (free * KD * b + (1.0 - free))
        return stiff, (acc, tuple(out))

    def first(n, c, rows, value, extra):
        free, inv = free_buf[n, rows], inv_buf[n, rows]
        r = free * (rhs_buf[n, c, rows] - value) - (1.0 - free) * u0_buf[n, c, rows]
        g = r * inv
        v_buf[0, n, c, rows] = g
        t_buf[1, 1 + n, c, rows] = free * g
        return extra[0] + r * g, extra[1]

    def held(rows, extra):
        return [stiff_buf[e, rows] for e in range(3)], extra

    def later(step):
        def finish(n, c, rows, value, extra):
            free, inv = free_buf[n, rows], inv_buf[n, rows]
            v = v_buf[step - 1, n, c, rows]
            w = free * value + (1.0 - free) * v
            new = w * inv
            v_buf[step, n, c, rows] = new
            t_buf[step + 1, 1 + n, c, rows] = free * new
            return extra + v * w if step == 1 else extra

        return finish

    gr = operate(0, stiffness, first, (zero8, (zero8, zero8)))[0]
    mark("mid0")
    zs.wait_recv()
    z_mix(0)
    ys = y_send(1, 0)
    count8 = zero8
    for n in range(2):
        for i in range(ROWS // 8):
            count8 = count8 + jnp.where(c_buf[1 + n, 8 * i : 8 * i + 8] > 0.0, 1.0, 0.0)
    gw = operate(1, held, later(1), zero8)

    mark("mid1")
    sums = [jnp.sum(t, axis=0, keepdims=True) for t in (gr, gw, count8)]
    sz_buf[0] = jnp.where(row == 0, sums[0], jnp.where(row == 1, sums[1], jnp.where(row == 2, sums[2], 0.0)))
    scalar_z = group(2, sz_buf, NZ_, lambda d: sz_buf.at[0], z_peer)
    ys.wait_recv()
    denom = y_sum(0)
    for a in range(2):
        den_buf[a] = denom[a]
        fz_buf[1, 0, a] = jnp.where(c_buf[1 + a, mine8] > 0.0, 1.0, 0.0) / denom[a]
    zs = z_send(3, 1)
    operate(2, held, later(2), 0)
    mark("mid2")
    scalar_z.wait_recv()
    sy_buf[0] = sum_of(sz_buf, NZ_)
    scalar_y = group(4, sy_buf, NY_, lambda d: sy_buf.at[0], y_peer)
    zs.wait_recv()
    z_mix(1)
    ys = y_send(5, 1)
    operate(3, held, later(3), 0)
    for step in range(1, SWEEPS):
        sent.append(whole(t_buf.at[step, 1:3, :, 0:ROWS], halo_send.at[step], halo_recv.at[step, 0]))
    sent.append(whole(t_buf.at[SWEEPS, 1, :, 0:ROWS], halo_send.at[SWEEPS], halo_recv.at[SWEEPS, 0]))

    mark("q8")
    ys.wait_recv()
    q8 = y_sum(1)
    for a in range(2):
        xq_buf[0, a] = q8[a]
    xs = group(6, xq_buf, RING, lambda d: xq_buf.at[0], lambda d: ring_peer(d)[1])

    mark("combine")
    scalar_y.wait_recv()
    tile = sum_of(sy_buf, NY_)
    gr_all = jnp.sum(tile[0:1], axis=1, keepdims=True)
    gw_all = jnp.sum(tile[1:2], axis=1, keepdims=True)
    count = jnp.sum(tile[2:3], axis=1, keepdims=True)
    coefs = [jnp.broadcast_to(c, (8, COLS)) for c in chebyshev(UPPER_FACTOR * gw_all / gr_all)]

    @pl.loop(0, ROWS // 8)
    def _(i):
        rows = pl.ds(pl.multiple_of(i * 8, 8), 8)
        for n in range(2):
            free = free_buf[n, rows]
            for c in range(3):
                u = u0_buf[n, c, rows]
                for power in range(SWEEPS):
                    u = u + coefs[power] * v_buf[power, n, c, rows]
                send_buf[n, c, rows] = u
                tu_buf[n, c, rows] = free * u

    def own_layer(n, c, rows):
        return tu_buf[n, c, rows]

    def upper_layer(n, c, rows):
        if n < 2:
            return tu_buf[n, c, rows]
        u = t_buf[0, 3, c, rows]
        for power in range(SWEEPS):
            u = u + coefs[power] * t_buf[power + 1, 3, c, rows]
        return u * has_above

    def energy_chunk(e, layer, i):
        rows = pl.ds(pl.multiple_of(i * 8, 8), 8)
        after = pl.ds(pl.multiple_of(i * 8 + 8, 8), 8)
        planes = [
            [plane_modes(layer(n, c, rows), layer(n, c, after), row, col) for c in range(3)]
            for n in (e, e + 1)
        ]
        value = cell_energy(cell_modes(*planes))
        weight = (3.0 * (1.0 - STIFF_VOID)) * c_buf[1 + e, rows]
        num_buf[e, rows] = weight * value

    def smooth_xy(plane):
        return dot(gauss_x, dot(plane, gauss_y))

    mark("energy0")

    @pl.loop(0, PIECES)
    def _(p):
        for part in range(PIECE // 8):
            energy_chunk(0, own_layer, p * (PIECE // 8) + part)

    rs0 = smooth_xy(num_buf[0])
    mark("waitq")
    xs.wait_recv()
    for d in range(RING):
        there = pl.ds(pl.multiple_of(8 * lax.rem(j + RING - d, RING), 8), 8)
        for a in range(2):
            q_buf[a, there] = xq_buf[d, a]
    mark("smoothq")
    for a in range(2):
        q_buf[a] = smooth_xy(q_buf[a])
    part0 = jnp.zeros((8, COLS), F32)
    for i in range(ROWS // 8):
        cut = slice(8 * i, 8 * i + 8)
        part0 = part0 + q_buf[0, cut] * num_buf[0, cut]
    smooth_buf2 = rs0

    mark("wait_last")

    def last_piece(p):
        whole(
            t_buf.at[SWEEPS, 3, :, piece(p)], halo_send.at[SWEEPS], halo_recv.at[SWEEPS, p]
        ).wait_recv()

    last_piece(0)

    @pl.loop(0, PIECES)
    def _(p):
        @pl.when(p < PIECES - 1)
        def _():
            last_piece(p + 1)

        for part in range(PIECE // 8):
            energy_chunk(1, upper_layer, p * (PIECE // 8) + part)

    mark("smoothn")
    rs1 = smooth_xy(num_buf[1])
    part = part0
    for i in range(ROWS // 8):
        cut = slice(8 * i, 8 * i + 8)
        part = part + q_buf[1, cut] * num_buf[1, cut]
    num_buf[0] = smooth_buf2
    num_buf[1] = rs1
    for a in range(2):
        rs_buf[0, a] = num_buf[a, mine8]
    xs = group(
        7, rs_buf, RING,
        lambda d: num_buf.at[:, pl.ds(pl.multiple_of(8 * ring_peer(d)[0], 8), 8)],
        lambda d: ring_peer(d)[1],
    )
    wx_buf[0] = jnp.sum(part, axis=0, keepdims=True)
    wxs = group(8, wx_buf, RING, lambda d: wx_buf.at[0], lambda d: ring_peer(d)[1])
    got_back = one(3, send_buf.at[other], back_buf, partner)
    for c in range(3):
        disp_out[h, c, 0] = send_buf[h, c]
    mark("wait_rs")
    xs.wait_recv()
    for a in range(2):
        total = rs_buf[0, a]
        for d in range(1, RING):
            total = total + rs_buf[d, a]
        fz_buf[2, 0, a] = total
    zs = z_send(9, 2)
    mark("wait_wx")
    wxs.wait_recv()
    wz_buf[0] = sum_of(wx_buf, RING)
    wzs = group(10, wz_buf, NZ_, lambda d: wz_buf.at[0], z_peer)
    mark("wait_z")
    zs.wait_recv()
    mark("zmix2")
    z_mix(2)
    ys = y_send(11, 2)
    mark("wait_wz")
    wzs.wait_recv()
    wy_buf[0] = sum_of(wz_buf, NZ_)
    wys = group(12, wy_buf, NY_, lambda d: wy_buf.at[0], y_peer)
    mark("wait_y")
    ys.wait_recv()
    numer = y_sum(2)
    mark("wait_wy")
    wys.wait_recv()
    mark("trial")
    weighted_all = jnp.sum(sum_of(wy_buf, NY_), axis=1, keepdims=True)
    inv_mean = 1.0 / (weighted_all / count + EPSILON)
    for a in range(2):
        here = jnp.where(c_buf[1 + a, mine8] > 0.0, 1.0, 0.0)
        weighted = here * (numer[a] / den_buf[a])
        ratio = weighted * inv_mean
        old = jnp.where(h == a, dens_ref[0, mine8], row_in[1])
        trial = jnp.minimum(
            jnp.maximum(old * jnp.sqrt(ratio), old - MOVE_LIMIT), old + MOVE_LIMIT
        )
        xt_buf[0, a] = here * trial
    xs = group(13, xt_buf, RING, lambda d: xt_buf.at[0], lambda d: ring_peer(d)[1])
    mark("wait_trial")
    xs.wait_recv()
    mark("volsum")
    tile = None
    for d in range(RING):
        for a in range(2):
            tile = xt_buf[d, a] if tile is None else tile + xt_buf[d, a]
    vol_buf[0] = jnp.sum(tile, axis=0, keepdims=True)
    vs = group(14, vol_buf, PLANE, lambda i: vol_buf.at[0], plane_peer)
    mark("wait_back")
    got_back.wait_recv()
    for c in range(3):
        disp_out[other, c, 0] = back_buf[c]
    for copy in sent[:-1]:
        copy.wait_send()
    mark("wait_vol")
    vs.wait_recv()
    mark("finish")
    volume = jnp.sum(sum_of(vol_buf, PLANE), axis=1, keepdims=True)
    scale = VOLUME_TARGET / (volume / count + EPSILON)
    for d in range(RING):
        there = pl.ds(pl.multiple_of(8 * lax.rem(j + RING - d, RING), 8), 8)
        dens_out[0, there] = jnp.minimum(scale * xt_buf[d, h], 1.0)
    vs.wait_send()
    mark(None)


def shards(start_disp, density, design, support, load_nodes, load_forces):
    vmem = lambda *shape: pltpu.VMEM(shape, F32)
    dma = lambda *shape: pltpu.SemaphoreType.DMA(shape)
    plane = (ROWS, COLS)
    return pl.pallas_call(
        kernel,
        out_shape=(
            jax.ShapeDtypeStruct(start_disp.shape, F32),
            jax.ShapeDtypeStruct(density.shape, F32),
        ),
        in_specs=[pl.BlockSpec(memory_space=pltpu.VMEM)] * 6,
        out_specs=(pl.BlockSpec(memory_space=pltpu.VMEM),) * 2,
        scratch_shapes=[
            vmem(SWEEPS + 1, 4, 3, ROWS + 8, COLS),
            vmem(SWEEPS, 2, 3, *plane),
            vmem(2, 3, *plane),
            vmem(2, 3, *plane),
            vmem(3, *plane),
            vmem(3, *plane),
            vmem(2, *plane),
            vmem(2, *plane),
            vmem(5, *plane),
            vmem(5, *plane),
            vmem(2, 3, ROWS + 8, COLS),
            vmem(2, 3, *plane),
            vmem(3, *plane),
            vmem(3 * NY_ * NZ_, 8, COLS),
            vmem(2, 8, COLS),
            vmem(2, 8, COLS),
            vmem(3, NZ_, 2, 8, COLS),
            vmem(3, NY_, 2, 8, COLS),
            vmem(3, NY_, 2, 8, COLS),
            vmem(*plane),
            vmem(RING, 2, 8, COLS),
            vmem(2, *plane),
            vmem(2, *plane),
            vmem(RING, 2, 8, COLS),
            vmem(RING, 2, 8, COLS),
            vmem(2, 8, COLS),
            vmem(NZ_, 8, COLS),
            vmem(NY_, 8, COLS),
            vmem(RING, 1, COLS),
            vmem(NZ_, 1, COLS),
            vmem(NY_, 1, COLS),
            vmem(PLANE, 1, COLS),
            dma(PIECES), dma(SWEEPS + 1, PIECES), dma(PIECES), dma(SWEEPS + 1),
            dma(4), dma(4), dma(15), dma(15),
        ],
        compiler_params=pltpu.CompilerParams(
            collective_id=0, has_side_effects=True, vmem_limit_bytes=48 * 1024 * 1024
        ),
    )(start_disp, density, design, support, load_nodes, jnp.transpose(load_forces, (1, 0, 2)))


def solution(mesh):
    return jax.shard_map(
        shards,
        mesh=mesh,
        in_specs=(
            P("load", None, "slab", None, None),
            P("slab", None, None),
            P("slab", None, None),
            P("slab", None, None),
            P("load", None),
            P("load", None, None),
        ),
        out_specs=(P("load", None, "slab", None, None), P("slab", None, None)),
        check_vma=False,
    )
```

```python
import contextlib

import jax
import jax.numpy as jnp
import numpy as np
from jax import lax
from jax.experimental import pallas as pl
from jax.experimental.pallas import tpu as pltpu
from jax.sharding import PartitionSpec as P

SWEEPS = 4
RADIUS = 2
POISSON = 0.3
STIFF_VOID = 0.001
UPPER_FACTOR = 1.2
LOWER_RATIO = 0.1
MOVE_LIMIT = 0.2
VOLUME_TARGET = 0.5
EPSILON = 1e-06
HIGHEST = lax.Precision.HIGHEST
MESH = pl.DeviceIdType.MESH
F32 = jnp.float32

NY_, NZ_ = 4, 8
LOADS_AX = 4
RING = 2 * LOADS_AX
PLANE = NY_ * NZ_
ROWS, COLS = 64, 128
POINTS = 2048
CHUNK = 256
PIECE = 16
PIECES = ROWS // PIECE


def hex_stiffness():
    lame_first = POISSON / ((1 + POISSON) * (1 - 2 * POISSON))
    lame_shear = 1 / (2 * (1 + POISSON))
    elastic = np.zeros((6, 6))
    elastic[:3, :3] = lame_first
    for axis_a in range(3):
        elastic[axis_a, axis_a] += 2 * lame_shear
        elastic[3 + axis_a, 3 + axis_a] = lame_shear
    shear_pairs = ((0, 1), (1, 2), (0, 2))
    gauss_point = 1 / np.sqrt(3)
    matrix = np.zeros((24, 24))
    for quad_index in range(8):
        quad_coords = [
            gauss_point * (2 * (quad_index >> 2 - axis_a & 1) - 1) for axis_a in range(3)
        ]
        shape_grads = np.zeros((8, 3))
        for corner in range(8):
            corner_signs = [2 * (corner >> 2 - axis_a & 1) - 1 for axis_a in range(3)]
            for axis_a in range(3):
                deriv_value = float(corner_signs[axis_a])
                for axis_b in range(3):
                    if axis_b != axis_a:
                        deriv_value *= (1 + corner_signs[axis_b] * quad_coords[axis_b]) / 2
                shape_grads[corner, axis_a] = deriv_value
        strain = np.zeros((6, 24))
        for corner in range(8):
            for axis_a in range(3):
                strain[axis_a, 3 * corner + axis_a] = shape_grads[corner, axis_a]
            for pair_index, shear_pair in enumerate(shear_pairs):
                strain[3 + pair_index, 3 * corner + shear_pair[0]] = shape_grads[
                    corner, shear_pair[1]
                ]
                strain[3 + pair_index, 3 * corner + shear_pair[1]] = shape_grads[
                    corner, shear_pair[0]
                ]
        matrix += strain.T @ elastic @ strain / 8
    return matrix.astype(np.float32)


def mode_stiffness():
    ke = hex_stiffness().astype(np.float64)
    w = np.zeros((24, 24))
    for p in range(8):
        for o in range(8):
            sign = 1.0
            for a in range(3):
                if p >> (2 - a) & 1:
                    sign *= 1.0 if o >> (2 - a) & 1 else -1.0
            for c in range(3):
                w[3 * p + c, 3 * o + c] = sign
    return w @ ke @ w.T / 64


KHAT = mode_stiffness()
KD = float(hex_stiffness()[0, 0])


def kh(p, c, q, d):
    return float(KHAT[3 * p + c, 3 * q + d])


SHEAR = kh(1, 0, 1, 0)
TRACE = kh(1, 2, 2, 1)
NORMAL = kh(1, 2, 1, 2) - TRACE
TWIST = kh(3, 0, 5, 1)
BEND = kh(3, 1, 3, 1)
CROSS = kh(3, 1, 5, 0)
LAST = kh(7, 0, 7, 0)

SHEAR_PAIRS = (((1, 0), (4, 2)), ((1, 1), (2, 2)), ((2, 0), (4, 1)))
NORMALS = ((4, 0), (2, 1), (1, 2))
TWISTS = ((3, 0), (5, 1), (6, 2))
BENDS = (((3, 1), (5, 0)), ((3, 2), (6, 0)), ((5, 2), (6, 1)))


def check_table():
    table = np.zeros((24, 24))

    def put(a, b, v):
        table[3 * a[0] + a[1], 3 * b[0] + b[1]] = v

    for a, b in SHEAR_PAIRS:
        for u in (a, b):
            for v in (a, b):
                put(u, v, SHEAR)
    for a in NORMALS:
        for b in NORMALS:
            put(a, b, TRACE + (NORMAL if a == b else 0))
    for a in TWISTS:
        for b in TWISTS:
            put(a, b, 2 * TWIST if a == b else TWIST)
    for a, b in BENDS:
        put(a, a, BEND)
        put(b, b, BEND)
        put(a, b, CROSS)
        put(b, a, CROSS)
    for c in range(3):
        put((7, c), (7, c), LAST)
    assert np.abs(table - KHAT).max() < 1e-8


check_table()


def shift_rows_up(v, after, row):
    return pltpu.roll(jnp.where(row == 0, after, v), 7, 0)


def plane_modes(v, after, row, col):
    ahead = shift_rows_up(v, after, row)
    out = {}
    for px, f in ((0, v + ahead), (1, ahead - v)):
        fa = jnp.where(col == COLS - 1, 0.0, pltpu.roll(f, COLS - 1, 1))
        out[px, 0] = f + fa
        out[px, 1] = fa - f
    return out


def cell_modes(bottom, top):
    m = {}
    for c in range(3):
        for p in range(1, 8):
            xy = (p >> 1 & 1, p & 1)
            b, t = bottom[c][xy], top[c][xy]
            m[p, c] = t - b if p >> 2 else t + b
    return m


def cell_forces(m, stiff):
    f = {}
    shear, trace, normal = stiff * SHEAR, stiff * TRACE, stiff * NORMAL
    twist, bend, cross, last = stiff * TWIST, stiff * BEND, stiff * CROSS, stiff * LAST
    for a, b in SHEAR_PAIRS:
        f[a] = f[b] = shear * (m[a] + m[b])
    total = trace * (m[NORMALS[0]] + m[NORMALS[1]] + m[NORMALS[2]])
    for a in NORMALS:
        f[a] = total + normal * m[a]
    total = m[TWISTS[0]] + m[TWISTS[1]] + m[TWISTS[2]]
    for a in TWISTS:
        f[a] = twist * (total + m[a])
    for a, b in BENDS:
        f[a] = bend * m[a] + cross * m[b]
        f[b] = cross * m[a] + bend * m[b]
    for c in range(3):
        f[7, c] = last * m[7, c]
    return f


def cell_energy(m):
    shear = None
    for a, b in SHEAR_PAIRS:
        s = m[a] + m[b]
        shear = s * s if shear is None else shear + s * s
    total = m[NORMALS[0]] + m[NORMALS[1]] + m[NORMALS[2]]
    normal = m[NORMALS[0]] * m[NORMALS[0]] + m[NORMALS[1]] * m[NORMALS[1]] + m[NORMALS[2]] * m[NORMALS[2]]
    twist = m[TWISTS[0]] + m[TWISTS[1]] + m[TWISTS[2]]
    twists = twist * twist
    for a in TWISTS:
        twists = twists + m[a] * m[a]
    bends = None
    crosses = None
    for a, b in BENDS:
        s = m[a] * m[a] + m[b] * m[b]
        t = m[a] * m[b]
        bends = s if bends is None else bends + s
        crosses = t if crosses is None else crosses + t
    last = m[7, 0] * m[7, 0] + m[7, 1] * m[7, 1] + m[7, 2] * m[7, 2]
    return (
        SHEAR * shear
        + TRACE * (total * total)
        + NORMAL * normal
        + TWIST * twists
        + BEND * bends
        + (2.0 * CROSS) * crosses
        + LAST * last
    )


def gauss(count):
    t = (
        lax.broadcasted_iota(jnp.int32, (count, count), 0)
        - lax.broadcasted_iota(jnp.int32, (count, count), 1)
    ).astype(F32) * (1.0 / RADIUS)
    return jnp.exp(-(t * t))


def dot(a, b):
    return lax.dot_general(
        a, b, (((1,), (0,)), ((), ())), precision=HIGHEST, preferred_element_type=F32
    )


def total_of(tile):
    return jnp.sum(jnp.sum(tile, axis=0, keepdims=True), axis=1, keepdims=True)


def chebyshev(upper):
    lower = LOWER_RATIO * upper
    center = 0.5 * (upper + lower)
    half_width = 0.5 * (upper - lower)
    spread = center / half_width
    factor = 1.0 / spread
    zero = jnp.zeros_like(upper)
    e = [jnp.ones_like(upper)] + [zero] * (SWEEPS - 1)
    d = [1.0 / center] + [zero] * (SWEEPS - 1)
    u = [zero] * SWEEPS
    for sweep in range(SWEEPS):
        u = [a + b for a, b in zip(u, d)]
        if sweep < SWEEPS - 1:
            e = [e[0]] + [e[n] - d[n - 1] for n in range(1, SWEEPS)]
            after = 1.0 / (2.0 * spread - factor)
            d = [after * factor * a + 2.0 * after / half_width * b for a, b in zip(d, e)]
            factor = after
    return u


def kernel(
    u0_hbm, dens_hbm, des_hbm, sup_hbm, nodes_hbm, forces_hbm,
    disp_out, dens_out,
    dens_ref, des_ref, sup_ref, nodes_ref, forces_ref,
    t_buf, v_buf, u0_buf, rhs_buf, c_buf, solid_buf, stiff_buf, inv_buf, free_buf,
    swap_out, swap_in, tu_buf, send_buf, back_buf, coef_buf, row_out, row_in,
    fz_buf, ps_buf, fy_buf, smooth_buf, num_buf, num2_buf, rs_buf, xt_buf, trial_buf,
    den_buf, sz_buf, wx_buf, wz_buf, vol_buf,
    load_sem, swap_recv, halo_recv, c_recv, halo_send, one_send, one_recv, group_send, group_recv,
):
    s = lax.axis_index("slab")
    l = lax.axis_index("load")
    h = lax.rem(s, 2)
    k = s // 2
    z = lax.rem(k, NZ_)
    y = k // NZ_
    j = h * LOADS_AX + l
    other = 1 - h

    def at(group, half=None, load=None):
        return {
            "slab": group * 2 + (h if half is None else half),
            "load": l if load is None else load,
        }

    above = lax.rem(k + 1, PLANE)
    below = lax.rem(k + PLANE - 1, PLANE)
    partner = at(k, half=other)

    def ring_peer(d):
        t = lax.rem(j + d, RING)
        return t, at(k, half=t // LOADS_AX, load=lax.rem(t, LOADS_AX))

    def z_peer(d):
        return at(y * NZ_ + lax.rem(z + d, NZ_))

    def y_peer(d):
        return at(lax.rem(y + d, NY_) * NZ_ + z)

    def plane_peer(i):
        return at(lax.rem(y + i // NZ_, NY_) * NZ_ + lax.rem(z + i % NZ_, NZ_))

    loads = [
        pltpu.make_async_copy(src, dst, load_sem.at[i])
        for i, (src, dst) in enumerate(
            (
                (u0_hbm.at[other, :, 0], swap_out.at[pl.ds(2, 3)]),
                (u0_hbm.at[h, :, 0], u0_buf.at[h]),
                (dens_hbm, dens_ref),
                (des_hbm, des_ref),
                (sup_hbm, sup_ref),
                (nodes_hbm, nodes_ref),
                (forces_hbm, forces_ref),
            )
        )
    ]
    for copy in loads:
        copy.start()

    phases = contextlib.ExitStack()

    def mark(name):
        phases.close()
        if name:
            phases.enter_context(jax.named_scope(name))

    mark("signals")
    barrier = pltpu.get_barrier_semaphore()
    for d in range(1, RING):
        pl.semaphore_signal(barrier, inc=1, device_id=ring_peer(d)[1], device_id_type=MESH)
    for i in range(1, PLANE):
        pl.semaphore_signal(barrier, inc=1, device_id=plane_peer(i), device_id_type=MESH)

    sent = []

    def start(src, dst, ss, rs, device):
        copy = pltpu.make_async_remote_copy(
            src_ref=src, dst_ref=dst, send_sem=ss, recv_sem=rs,
            device_id=device, device_id_type=MESH,
        )
        copy.start()
        return copy

    def whole(ref, ss, rs):
        return pltpu.make_async_remote_copy(
            src_ref=ref, dst_ref=ref, send_sem=ss, recv_sem=rs,
            device_id=partner, device_id_type=MESH,
        )

    def one(slot, src, dst, device):
        copy = start(src, dst, one_send.at[slot], one_recv.at[slot], device)
        sent.append(copy)
        return copy

    def group(slot, buf, count, src, peer):
        for d in range(1, count):
            start(src(d), buf.at[d], group_send.at[slot], group_recv.at[slot], peer(d))
        rest = whole(buf.at[pl.ds(1, count - 1)], group_send.at[slot], group_recv.at[slot])
        sent.append(rest)
        return rest

    row = lax.broadcasted_iota(jnp.int32, (8, COLS), 0)
    col = lax.broadcasted_iota(jnp.int32, (8, COLS), 1)
    zero8 = jnp.zeros((8, COLS), F32)

    @pl.loop(0, NY_ * NZ_)
    def _(i):
        dy, dz = i // NZ_, lax.rem(i, NZ_)
        offset = 16 * (lax.rem(y + dy, NY_) - y) + 2 * (z - lax.rem(z + NZ_ - dz, NZ_))
        for a in range(3):
            t = jnp.full((8, COLS), offset + (a - 1), jnp.int32).astype(F32) * (1.0 / RADIUS)
            coef_buf[i * 3 + a] = jnp.exp(-(t * t))

    mark("prep")
    for step in range(SWEEPS + 1):
        for n in range(4):
            for c in range(3):
                t_buf[step, n, c, ROWS : ROWS + 8] = zero8
    for n in range(2):
        for c in range(3):
            tu_buf[n, c, ROWS : ROWS + 8] = zero8
    gauss_x, gauss_y = gauss(ROWS), gauss(COLS)
    for copy in loads:
        copy.wait()
    dens = dens_ref[0]
    solid = des_ref[0].astype(F32) * dens
    cube = solid * solid * solid
    free_own = 1.0 - sup_ref[0].astype(F32)
    c_buf[1 + h] = cube
    free_buf[h] = free_own
    solid_buf[h] = solid
    swap_out[0] = solid
    swap_out[1] = free_own
    for c in range(3):
        t_buf[0, 1 + h, c, 0:ROWS] = u0_buf[h, c] * free_own
    smooth_buf[...] = dot(dot(gauss_x, dens), gauss_y)
    mine8 = pl.ds(pl.multiple_of(8 * j, 8), 8)
    other8 = pl.ds(pl.multiple_of(8 * (other * LOADS_AX + l), 8), 8)
    fz_buf[0, 0, h] = smooth_buf[mine8]
    row_out[...] = smooth_buf[other8]

    mark("barrier")
    pl.semaphore_wait(barrier, RING - 1 + PLANE - 1)

    mark("sends0")
    toward = jnp.where(h == 0, below, above)
    away = jnp.where(h == 0, above, below)

    def piece(p):
        if isinstance(p, int):
            return pl.ds(p * PIECE, PIECE)
        return pl.ds(pl.multiple_of(p * PIECE, PIECE), PIECE)

    got_rows = one(1, row_out, row_in, partner)
    for p in range(PIECES):
        start(
            swap_out.at[:, piece(p)], swap_in.at[:, piece(p)],
            one_send.at[0], swap_recv.at[p], partner,
        )
    sent.append(whole(swap_out, one_send.at[0], swap_recv.at[0]))
    for p in range(PIECES):
        start(
            t_buf.at[0, 1 + h, :, piece(p)], t_buf.at[0, 3 * other, :, piece(p)],
            halo_send.at[0], halo_recv.at[0, p], at(toward),
        )

    mark("rhs")
    base = k * (2 * ROWS)
    line = lax.broadcasted_iota(jnp.int32, (2 * ROWS, CHUNK), 0)
    for n in range(2):
        for c in range(3):
            rhs_buf[n, c] = jnp.zeros((ROWS, COLS), F32)

    @pl.loop(0, POINTS // CHUNK)
    def _(i):
        cut = pl.ds(pl.multiple_of(i * CHUNK, CHUNK), CHUNK)
        node = jnp.where(h == 0, nodes_ref[0:1, cut], nodes_ref[1:2, cut])
        place = jnp.where((node >> 7) - base == line, 1.0, 0.0).astype(jnp.bfloat16)
        across = (node & 127) == line
        for c in range(3):
            force = jnp.where(h == 0, forces_ref[c, 0:1, cut], forces_ref[c, 1:2, cut])
            spread = jnp.where(across, force, 0.0)
            total = jnp.zeros((2 * ROWS, COLS), F32)
            for part in range(3):
                bits = spread.astype(jnp.bfloat16)
                total = total + lax.dot_general(
                    place, bits, (((1,), (1,)), ((), ())), preferred_element_type=F32
                )
                if part < 2:
                    spread = spread - bits.astype(F32)
            rhs_buf[0, c] += total[:ROWS]
            rhs_buf[1, c] += total[ROWS:]

    def z_send(slot, which):
        return group(slot, fz_buf.at[which], NZ_, lambda d: fz_buf.at[which, 0], z_peer)

    def z_mix(which):
        @pl.loop(0, NY_)
        def _(dy):
            for a in range(2):
                total = None
                for d in range(NZ_):
                    for b in range(2):
                        term = coef_buf[dy * (3 * NZ_) + (3 * d + a - b + 1)] * fz_buf[which, d, b]
                        total = term if total is None else total + term
                ps_buf[which, dy, a] = total

        for a in range(2):
            fy_buf[which, 0, a] = ps_buf[which, 0, a]

    def y_send(slot, which):
        return group(slot, fy_buf.at[which], NY_, lambda d: ps_buf.at[which, d], y_peer)

    def y_sum(which):
        return [
            fy_buf[which, 0, a] + fy_buf[which, 1, a] + fy_buf[which, 2, a] + fy_buf[which, 3, a]
            for a in range(2)
        ]

    def sum_of(buf, count):
        tile = buf[0]
        for d in range(1, count):
            tile = tile + buf[d]
        return tile

    mark("rows")
    got_rows.wait_recv()
    fz_buf[0, 0, other] = row_in[...]
    zs = z_send(0, 0)

    mark("forward")

    @pl.loop(0, PIECES)
    def _(p):
        rows = piece(p)
        whole(swap_in.at[:, rows], one_send.at[0], swap_recv.at[p]).wait_recv()
        free = swap_in[1, rows]
        free_buf[other, rows] = free
        part = swap_in[0, rows]
        solid_buf[other, rows] = part
        c_buf[1 + other, rows] = part * part * part
        for c in range(3):
            u = swap_in[2 + c, rows]
            u0_buf[other, c, rows] = u
            t_buf[0, 1 + other, c, rows] = u * free
        start(c_buf.at[2, rows], c_buf.at[0, rows], one_send.at[2], c_recv.at[p], at(above))
        start(
            t_buf.at[0, 1 + other, :, rows], t_buf.at[0, 3 * h, :, rows],
            halo_send.at[0], halo_recv.at[0, p], at(away),
        )

    sent.append(whole(c_buf.at[0], one_send.at[2], c_recv.at[0]))
    sent.append(whole(t_buf.at[0, 1:3, :, 0:ROWS], halo_send.at[0], halo_recv.at[0, 0]))
    has_below = jnp.where(k > 0, 1.0, 0.0)
    has_above = jnp.where(k < PLANE - 1, 1.0, 0.0)

    def wait_piece(step, p):
        if step == 0:
            whole(c_buf.at[0, piece(p)], one_send.at[2], c_recv.at[p]).wait_recv()
        whole(
            t_buf.at[step, 1:3, :, piece(p)], halo_send.at[step], halo_recv.at[step, p]
        ).wait_recv()

    def operate(step, before, finish, extra, meanwhile=None):
        def chunk(i, behind, extra):
            behind = list(behind)
            rows = pl.ds(pl.multiple_of(i * 8, 8), 8)
            after = pl.ds(pl.multiple_of(i * 8 + 8, 8), 8)
            stiff, extra = before(rows, extra)
            total = [None, None]
            lower = None
            for n in range(4):
                upper = []
                for c in range(3):
                    v, w = t_buf[step, n, c, rows], t_buf[step, n, c, after]
                    if n == 3:
                        v, w = v * has_above, w * has_above
                    upper.append(plane_modes(v, w, row, col))
                if n:
                    e = n - 1
                    f = cell_forces(cell_modes(lower, upper), stiff[e])
                    for node, sign in ((e, 1.0), (e - 1, -1.0)):
                        if not 0 <= node < 2:
                            continue
                        part = {}
                        for c in range(3):
                            for q in range(4):
                                hi = f[4 + q, c]
                                if q == 0:
                                    value = hi if sign > 0 else -hi
                                else:
                                    value = f[q, c] + hi if sign > 0 else f[q, c] - hi
                                part[c, q] = value
                        if total[node] is None:
                            total[node] = part
                        else:
                            total[node] = {key: total[node][key] + part[key] for key in part}
                lower = upper
            for node in range(2):
                for c in range(3):
                    g = []
                    for px in range(2):
                        fs, fd = total[node][c, 2 * px], total[node][c, 2 * px + 1]
                        shifted = jnp.where(col == 0, 0.0, pltpu.roll(fs + fd, 1, 1))
                        g.append(fs - fd + shifted)
                    r = pltpu.roll(g[0] + g[1], 1, 0)
                    slot = 3 * node + c
                    value = g[0] - g[1] + jnp.where(row == 0, behind[slot], r)
                    behind[slot] = r
                    extra = finish(node, c, rows, value, extra)
            return tuple(behind), extra

        def body(p, carry):
            behind, extra = carry

            @pl.when(p < PIECES - 1)
            def _():
                wait_piece(step, p + 1)

            for part in range(PIECE // 8):
                behind, extra = chunk(p * (PIECE // 8) + part, behind, extra)
            send_piece(step + 1, p)
            return behind, extra

        mark(f"wait{step}")
        wait_piece(step, 0)
        if meanwhile:
            meanwhile()
        mark(f"app{step}")
        out = lax.fori_loop(0, PIECES, body, ((zero8,) * 6, extra))[1]
        return out

    def send_piece(step, p):
        rows = piece(p)
        if step < SWEEPS:
            start(
                t_buf.at[step, 2, :, rows], t_buf.at[step, 0, :, rows],
                halo_send.at[step], halo_recv.at[step, p], at(above),
            )
        start(
            t_buf.at[step, 1, :, rows], t_buf.at[step, 3, :, rows],
            halo_send.at[step], halo_recv.at[step, p], at(below),
        )

    def stiffness(rows, extra):
        acc, rolls = extra
        stiff = [STIFF_VOID + (1.0 - STIFF_VOID) * c_buf[e, rows] for e in range(3)]
        stiff[0] = stiff[0] * has_below
        out = []
        for e in range(3):
            stiff_buf[e, rows] = stiff[e]
        for n in range(2):
            b = stiff[n] + stiff[n + 1]
            b = b + jnp.where(col == 0, 0.0, pltpu.roll(b, 1, 1))
            r = pltpu.roll(b, 1, 0)
            b = b + jnp.where(row == 0, rolls[n], r)
            out.append(r)
            free = free_buf[n, rows]
            inv_buf[n, rows] = 1.0 / (free * KD * b + (1.0 - free))
        return stiff, (acc, tuple(out))

    def first(n, c, rows, value, extra):
        free, inv = free_buf[n, rows], inv_buf[n, rows]
        r = free * (rhs_buf[n, c, rows] - value) - (1.0 - free) * u0_buf[n, c, rows]
        g = r * inv
        v_buf[0, n, c, rows] = g
        t_buf[1, 1 + n, c, rows] = free * g
        return extra[0] + r * g, extra[1]

    def held(rows, extra):
        return [stiff_buf[e, rows] for e in range(3)], extra

    def later(step):
        def finish(n, c, rows, value, extra):
            free, inv = free_buf[n, rows], inv_buf[n, rows]
            v = v_buf[step - 1, n, c, rows]
            w = free * value + (1.0 - free) * v
            new = w * inv
            v_buf[step, n, c, rows] = new
            t_buf[step + 1, 1 + n, c, rows] = free * new
            return extra + v * w if step == 1 else extra

        return finish

    gr = operate(0, stiffness, first, (zero8, (zero8, zero8)))[0]
    mark("mid0")
    zs.wait_recv()
    z_mix(0)
    ys = y_send(1, 0)
    count8 = zero8
    for n in range(2):
        for i in range(ROWS // 8):
            count8 = count8 + jnp.where(solid_buf[n, 8 * i : 8 * i + 8] > 0.0, 1.0, 0.0)
    gw = operate(1, held, later(1), zero8)

    mark("mid1")
    lane = lax.broadcasted_iota(jnp.int32, (1, COLS), 1)
    line0 = jnp.zeros((1, COLS), F32)
    for i, tile in enumerate((gr, gw, count8)):
        line0 = jnp.where(lane == i, total_of(tile), line0)
    sz_buf[0] = line0
    scalars = group(2, sz_buf, PLANE, lambda i: sz_buf.at[0], plane_peer)
    ys.wait_recv()
    denom = y_sum(0)
    for a in range(2):
        den_buf[a] = denom[a]
        fz_buf[1, 0, a] = jnp.where(solid_buf[a, mine8] > 0.0, 1.0, 0.0) / denom[a]
    zs = z_send(3, 1)
    operate(2, held, later(2), 0)
    q_flight = []

    def q_mix():
        zs.wait_recv()
        z_mix(1)
        q_flight.append(y_send(5, 1))

    operate(3, held, later(3), 0, q_mix)
    for step in range(1, SWEEPS):
        sent.append(whole(t_buf.at[step, 1:3, :, 0:ROWS], halo_send.at[step], halo_recv.at[step, 0]))
    sent.append(whole(t_buf.at[SWEEPS, 1, :, 0:ROWS], halo_send.at[SWEEPS], halo_recv.at[SWEEPS, 0]))

    mark("combine")
    scalars.wait_recv()
    line0 = sum_of(sz_buf, PLANE)
    gr_all, gw_all, count = line0[:, 0:1], line0[:, 1:2], line0[:, 2:3]
    coefs = [jnp.broadcast_to(c, (8, COLS)) for c in chebyshev(UPPER_FACTOR * gw_all / gr_all)]

    @pl.loop(0, ROWS // 8)
    def _(i):
        rows = pl.ds(pl.multiple_of(i * 8, 8), 8)
        for n in range(2):
            free = free_buf[n, rows]
            for c in range(3):
                u = u0_buf[n, c, rows]
                for power in range(SWEEPS):
                    u = u + coefs[power] * v_buf[power, n, c, rows]
                send_buf[n, c, rows] = u
                tu_buf[n, c, rows] = free * u

    def own_layer(n, c, rows):
        return tu_buf[n, c, rows]

    def upper_layer(n, c, rows):
        if n < 2:
            return tu_buf[n, c, rows]
        u = t_buf[0, 3, c, rows]
        for power in range(SWEEPS):
            u = u + coefs[power] * t_buf[power + 1, 3, c, rows]
        return u * has_above

    def energy_chunk(e, layer, i):
        rows = pl.ds(pl.multiple_of(i * 8, 8), 8)
        after = pl.ds(pl.multiple_of(i * 8 + 8, 8), 8)
        planes = [
            [plane_modes(layer(n, c, rows), layer(n, c, after), row, col) for c in range(3)]
            for n in (e, e + 1)
        ]
        value = cell_energy(cell_modes(*planes))
        weight = (3.0 * (1.0 - STIFF_VOID)) * c_buf[1 + e, rows]
        num_buf[e, rows] = weight * value

    def smooth_xy(plane):
        return dot(gauss_x, dot(plane, gauss_y))

    mark("energy0")

    @pl.loop(0, PIECES)
    def _(p):
        for part in range(PIECE // 8):
            energy_chunk(0, own_layer, p * (PIECE // 8) + part)

    rs0 = smooth_xy(num_buf[0])
    mark("wait_last")

    def last_piece(p):
        whole(
            t_buf.at[SWEEPS, 3, :, piece(p)], halo_send.at[SWEEPS], halo_recv.at[SWEEPS, p]
        ).wait_recv()

    last_piece(0)

    @pl.loop(0, PIECES)
    def _(p):
        @pl.when(p < PIECES - 1)
        def _():
            last_piece(p + 1)

        for part in range(PIECE // 8):
            energy_chunk(1, upper_layer, p * (PIECE // 8) + part)

    mark("smoothn")
    rs1 = smooth_xy(num_buf[1])
    num2_buf[0] = rs0
    num2_buf[1] = rs1
    for a in range(2):
        rs_buf[0, a] = num2_buf[a, mine8]
    xs = group(
        7, rs_buf, RING,
        lambda d: num2_buf.at[:, pl.ds(pl.multiple_of(8 * ring_peer(d)[0], 8), 8)],
        lambda d: ring_peer(d)[1],
    )
    mark("wait_rs")
    xs.wait_recv()
    totals = [sum_of(rs_buf.at[:, a], RING) for a in range(2)]
    for a in range(2):
        fz_buf[2, 0, a] = totals[a]
    zs = z_send(9, 2)
    mark("wpart")
    q_flight[0].wait_recv()
    q8 = y_sum(1)
    wx_buf[0] = jnp.sum(q8[0] * totals[0] + q8[1] * totals[1], axis=0, keepdims=True)
    wxs = group(8, wx_buf, RING, lambda d: wx_buf.at[0], lambda d: ring_peer(d)[1])
    got_back = one(3, send_buf.at[other], back_buf, partner)
    for c in range(3):
        disp_out[h, c, 0] = send_buf[h, c]
    mark("wait_wx")
    wxs.wait_recv()
    wz_buf[0] = sum_of(wx_buf, RING)
    wzs = group(10, wz_buf, PLANE, lambda i: wz_buf.at[0], plane_peer)
    mark("wait_z")
    zs.wait_recv()
    mark("zmix2")
    z_mix(2)
    ys = y_send(11, 2)
    mark("wait_y")
    ys.wait_recv()
    numer = y_sum(2)
    for a in range(2):
        here = jnp.where(solid_buf[a, mine8] > 0.0, 1.0, 0.0)
        xt_buf[0, a] = here * (numer[a] / den_buf[a])
    xs = group(13, xt_buf, RING, lambda d: xt_buf.at[0], lambda d: ring_peer(d)[1])
    mark("wait_wz")
    wzs.wait_recv()
    weighted_all = jnp.sum(sum_of(wz_buf, PLANE), axis=1, keepdims=True)
    inv_mean = 1.0 / (weighted_all / count + EPSILON)
    mark("wait_x")
    xs.wait_recv()
    mark("trial")
    tile = zero8
    for d in range(RING):
        there = pl.ds(pl.multiple_of(8 * lax.rem(j + RING - d, RING), 8), 8)
        for a in range(2):
            old = solid_buf[a, there]
            trial = jnp.minimum(
                jnp.maximum(old * jnp.sqrt(xt_buf[d, a] * inv_mean), old - MOVE_LIMIT),
                old + MOVE_LIMIT,
            )
            tile = tile + trial
            trial_buf[a, there] = trial
    vol_buf[0] = jnp.sum(tile, axis=0, keepdims=True)
    vs = group(14, vol_buf, PLANE, lambda i: vol_buf.at[0], plane_peer)
    mark("wait_back")
    got_back.wait_recv()
    for c in range(3):
        disp_out[other, c, 0] = back_buf[c]
    for copy in sent[:-1]:
        copy.wait_send()
    mark("wait_vol")
    vs.wait_recv()
    mark("finish")
    volume = jnp.sum(sum_of(vol_buf, PLANE), axis=1, keepdims=True)
    scale = VOLUME_TARGET / (volume / count + EPSILON)
    dens_out[0] = jnp.minimum(scale * trial_buf[h], 1.0)
    vs.wait_send()
    mark(None)


def shards(start_disp, density, design, support, load_nodes, load_forces):
    arrays = (
        start_disp, density, design, support, load_nodes, jnp.transpose(load_forces, (1, 0, 2)),
    )
    vmem = lambda *shape: pltpu.VMEM(shape, F32)
    dma = lambda *shape: pltpu.SemaphoreType.DMA(shape)
    plane = (ROWS, COLS)
    return pl.pallas_call(
        kernel,
        out_shape=(
            pltpu.VMEM(start_disp.shape, F32),
            pltpu.VMEM(density.shape, F32),
        ),
        in_specs=[pl.BlockSpec(memory_space=pltpu.HBM)] * 6,
        out_specs=(pl.BlockSpec(memory_space=pltpu.VMEM),) * 2,
        scratch_shapes=[
            vmem(1, *plane),
            pltpu.VMEM((1, *plane), jnp.int32),
            pltpu.VMEM((1, *plane), jnp.int32),
            pltpu.VMEM((2, POINTS), jnp.int32),
            vmem(3, 2, POINTS),
            vmem(SWEEPS + 1, 4, 3, ROWS + 8, COLS),
            vmem(SWEEPS, 2, 3, *plane),
            vmem(2, 3, *plane),
            vmem(2, 3, *plane),
            vmem(3, *plane),
            vmem(2, *plane),
            vmem(3, *plane),
            vmem(2, *plane),
            vmem(2, *plane),
            vmem(5, *plane),
            vmem(5, *plane),
            vmem(2, 3, ROWS + 8, COLS),
            vmem(2, 3, *plane),
            vmem(3, *plane),
            vmem(3 * NY_ * NZ_, 8, COLS),
            vmem(8, COLS),
            vmem(8, COLS),
            vmem(3, NZ_, 2, 8, COLS),
            vmem(3, NY_, 2, 8, COLS),
            vmem(3, NY_, 2, 8, COLS),
            vmem(*plane),
            vmem(2, *plane),
            vmem(2, *plane),
            vmem(RING, 2, 8, COLS),
            vmem(RING, 2, 8, COLS),
            vmem(2, *plane),
            vmem(2, 8, COLS),
            vmem(PLANE, 1, COLS),
            vmem(RING, 1, COLS),
            vmem(PLANE, 1, COLS),
            vmem(PLANE, 1, COLS),
            dma(7), dma(PIECES), dma(SWEEPS + 1, PIECES), dma(PIECES), dma(SWEEPS + 1),
            dma(4), dma(4), dma(15), dma(15),
        ],
        compiler_params=pltpu.CompilerParams(
            collective_id=0, has_side_effects=True, vmem_limit_bytes=48 * 1024 * 1024
        ),
    )(*(pltpu.with_memory_space_constraint(a, pltpu.HBM) for a in arrays))


def solution(mesh):
    return jax.shard_map(
        shards,
        mesh=mesh,
        in_specs=(
            P("load", None, "slab", None, None),
            P("slab", None, None),
            P("slab", None, None),
            P("slab", None, None),
            P("load", None),
            P("load", None, None),
        ),
        out_specs=(P("load", None, "slab", None, None), P("slab", None, None)),
        check_vma=False,
    )
```

```python
import contextlib

import jax
import jax.numpy as jnp
import numpy as np
from jax import lax
from jax.experimental import pallas as pl
from jax.experimental.pallas import tpu as pltpu
from jax.sharding import PartitionSpec as P

SWEEPS = 4
RADIUS = 2
POISSON = 0.3
STIFF_VOID = 0.001
UPPER_FACTOR = 1.2
LOWER_RATIO = 0.1
MOVE_LIMIT = 0.2
VOLUME_TARGET = 0.5
EPSILON = 1e-06
HIGHEST = lax.Precision.HIGHEST
MESH = pl.DeviceIdType.MESH
F32 = jnp.float32

NY_, NZ_ = 4, 8
LOADS_AX = 4
RING = 2 * LOADS_AX
PLANE = NY_ * NZ_
ROWS, COLS = 64, 128
POINTS = 2048
CHUNK = 256
PIECES = 5


def hex_stiffness():
    lame_first = POISSON / ((1 + POISSON) * (1 - 2 * POISSON))
    lame_shear = 1 / (2 * (1 + POISSON))
    elastic = np.zeros((6, 6))
    elastic[:3, :3] = lame_first
    for axis_a in range(3):
        elastic[axis_a, axis_a] += 2 * lame_shear
        elastic[3 + axis_a, 3 + axis_a] = lame_shear
    shear_pairs = ((0, 1), (1, 2), (0, 2))
    gauss_point = 1 / np.sqrt(3)
    matrix = np.zeros((24, 24))
    for quad_index in range(8):
        quad_coords = [
            gauss_point * (2 * (quad_index >> 2 - axis_a & 1) - 1) for axis_a in range(3)
        ]
        shape_grads = np.zeros((8, 3))
        for corner in range(8):
            corner_signs = [2 * (corner >> 2 - axis_a & 1) - 1 for axis_a in range(3)]
            for axis_a in range(3):
                deriv_value = float(corner_signs[axis_a])
                for axis_b in range(3):
                    if axis_b != axis_a:
                        deriv_value *= (1 + corner_signs[axis_b] * quad_coords[axis_b]) / 2
                shape_grads[corner, axis_a] = deriv_value
        strain = np.zeros((6, 24))
        for corner in range(8):
            for axis_a in range(3):
                strain[axis_a, 3 * corner + axis_a] = shape_grads[corner, axis_a]
            for pair_index, shear_pair in enumerate(shear_pairs):
                strain[3 + pair_index, 3 * corner + shear_pair[0]] = shape_grads[
                    corner, shear_pair[1]
                ]
                strain[3 + pair_index, 3 * corner + shear_pair[1]] = shape_grads[
                    corner, shear_pair[0]
                ]
        matrix += strain.T @ elastic @ strain / 8
    return matrix.astype(np.float32)


def mode_stiffness():
    ke = hex_stiffness().astype(np.float64)
    w = np.zeros((24, 24))
    for p in range(8):
        for o in range(8):
            sign = 1.0
            for a in range(3):
                if p >> (2 - a) & 1:
                    sign *= 1.0 if o >> (2 - a) & 1 else -1.0
            for c in range(3):
                w[3 * p + c, 3 * o + c] = sign
    return w @ ke @ w.T / 64


KHAT = mode_stiffness()
KD = float(hex_stiffness()[0, 0])


def kh(p, c, q, d):
    return float(KHAT[3 * p + c, 3 * q + d])


SHEAR = kh(1, 0, 1, 0)
TRACE = kh(1, 2, 2, 1)
NORMAL = kh(1, 2, 1, 2) - TRACE
TWIST = kh(3, 0, 5, 1)
BEND = kh(3, 1, 3, 1)
CROSS = kh(3, 1, 5, 0)
LAST = kh(7, 0, 7, 0)

SHEAR_PAIRS = (((1, 0), (4, 2)), ((1, 1), (2, 2)), ((2, 0), (4, 1)))
NORMALS = ((4, 0), (2, 1), (1, 2))
TWISTS = ((3, 0), (5, 1), (6, 2))
BENDS = (((3, 1), (5, 0)), ((3, 2), (6, 0)), ((5, 2), (6, 1)))


def check_table():
    table = np.zeros((24, 24))

    def put(a, b, v):
        table[3 * a[0] + a[1], 3 * b[0] + b[1]] = v

    for a, b in SHEAR_PAIRS:
        for u in (a, b):
            for v in (a, b):
                put(u, v, SHEAR)
    for a in NORMALS:
        for b in NORMALS:
            put(a, b, TRACE + (NORMAL if a == b else 0))
    for a in TWISTS:
        for b in TWISTS:
            put(a, b, 2 * TWIST if a == b else TWIST)
    for a, b in BENDS:
        put(a, a, BEND)
        put(b, b, BEND)
        put(a, b, CROSS)
        put(b, a, CROSS)
    for c in range(3):
        put((7, c), (7, c), LAST)
    assert np.abs(table - KHAT).max() < 1e-8


check_table()


def shift_rows_up(v, after, row):
    return pltpu.roll(jnp.where(row == 0, after, v), 7, 0)


def plane_modes(v, after, row, col):
    ahead = shift_rows_up(v, after, row)
    out = {}
    for px, f in ((0, v + ahead), (1, ahead - v)):
        fa = jnp.where(col == COLS - 1, 0.0, pltpu.roll(f, COLS - 1, 1))
        out[px, 0] = f + fa
        out[px, 1] = fa - f
    return out


def cell_modes(bottom, top):
    m = {}
    for c in range(3):
        for p in range(1, 8):
            xy = (p >> 1 & 1, p & 1)
            b, t = bottom[c][xy], top[c][xy]
            m[p, c] = t - b if p >> 2 else t + b
    return m


def cell_forces(m, stiff):
    f = {}
    shear, trace, normal = stiff * SHEAR, stiff * TRACE, stiff * NORMAL
    twist, bend, cross, last = stiff * TWIST, stiff * BEND, stiff * CROSS, stiff * LAST
    for a, b in SHEAR_PAIRS:
        f[a] = f[b] = shear * (m[a] + m[b])
    total = trace * (m[NORMALS[0]] + m[NORMALS[1]] + m[NORMALS[2]])
    for a in NORMALS:
        f[a] = total + normal * m[a]
    total = m[TWISTS[0]] + m[TWISTS[1]] + m[TWISTS[2]]
    for a in TWISTS:
        f[a] = twist * (total + m[a])
    for a, b in BENDS:
        f[a] = bend * m[a] + cross * m[b]
        f[b] = cross * m[a] + bend * m[b]
    for c in range(3):
        f[7, c] = last * m[7, c]
    return f


def cell_energy(m):
    shear = None
    for a, b in SHEAR_PAIRS:
        s = m[a] + m[b]
        shear = s * s if shear is None else shear + s * s
    total = m[NORMALS[0]] + m[NORMALS[1]] + m[NORMALS[2]]
    normal = m[NORMALS[0]] * m[NORMALS[0]] + m[NORMALS[1]] * m[NORMALS[1]] + m[NORMALS[2]] * m[NORMALS[2]]
    twist = m[TWISTS[0]] + m[TWISTS[1]] + m[TWISTS[2]]
    twists = twist * twist
    for a in TWISTS:
        twists = twists + m[a] * m[a]
    bends = None
    crosses = None
    for a, b in BENDS:
        s = m[a] * m[a] + m[b] * m[b]
        t = m[a] * m[b]
        bends = s if bends is None else bends + s
        crosses = t if crosses is None else crosses + t
    last = m[7, 0] * m[7, 0] + m[7, 1] * m[7, 1] + m[7, 2] * m[7, 2]
    return (
        SHEAR * shear
        + TRACE * (total * total)
        + NORMAL * normal
        + TWIST * twists
        + BEND * bends
        + (2.0 * CROSS) * crosses
        + LAST * last
    )


def gauss(count):
    t = (
        lax.broadcasted_iota(jnp.int32, (count, count), 0)
        - lax.broadcasted_iota(jnp.int32, (count, count), 1)
    ).astype(F32) * (1.0 / RADIUS)
    return jnp.exp(-(t * t))


def dot(a, b):
    return lax.dot_general(
        a, b, (((1,), (0,)), ((), ())), precision=HIGHEST, preferred_element_type=F32
    )


def total_of(tile):
    return jnp.sum(jnp.sum(tile, axis=0, keepdims=True), axis=1, keepdims=True)


def chebyshev(upper):
    lower = LOWER_RATIO * upper
    center = 0.5 * (upper + lower)
    half_width = 0.5 * (upper - lower)
    spread = center / half_width
    factor = 1.0 / spread
    zero = jnp.zeros_like(upper)
    e = [jnp.ones_like(upper)] + [zero] * (SWEEPS - 1)
    d = [1.0 / center] + [zero] * (SWEEPS - 1)
    u = [zero] * SWEEPS
    for sweep in range(SWEEPS):
        u = [a + b for a, b in zip(u, d)]
        if sweep < SWEEPS - 1:
            e = [e[0]] + [e[n] - d[n - 1] for n in range(1, SWEEPS)]
            after = 1.0 / (2.0 * spread - factor)
            d = [after * factor * a + 2.0 * after / half_width * b for a, b in zip(d, e)]
            factor = after
    return u


def kernel(
    u0_hbm, dens_hbm, des_hbm, sup_hbm, nodes_hbm, forces_hbm,
    disp_out, dens_out,
    dens_ref, des_ref, sup_ref, nodes_ref, forces_ref,
    t_buf, v_buf, u0_buf, rhs_buf, c_buf, solid_buf, stiff_buf, inv_buf, free_buf,
    swap_out, swap_in, tu_buf, send_buf, back_buf, coef_buf, row_out, row_in,
    fz_buf, ps_buf, fy_buf, smooth_buf, num_buf, num2_buf, rs_buf, xt_buf, trial_buf,
    den_buf, sz_buf, wx_buf, wz_buf, vol_buf,
    load_sem, swap_recv, halo_recv, c_recv, halo_send, one_send, one_recv, group_send, group_recv,
):
    s = lax.axis_index("slab")
    l = lax.axis_index("load")
    h = lax.rem(s, 2)
    k = s // 2
    z = lax.rem(k, NZ_)
    y = k // NZ_
    j = h * LOADS_AX + l
    other = 1 - h

    def at(group, half=None, load=None):
        return {
            "slab": group * 2 + (h if half is None else half),
            "load": l if load is None else load,
        }

    above = lax.rem(k + 1, PLANE)
    below = lax.rem(k + PLANE - 1, PLANE)
    partner = at(k, half=other)

    def ring_peer(d):
        t = lax.rem(j + d, RING)
        return t, at(k, half=t // LOADS_AX, load=lax.rem(t, LOADS_AX))

    def z_peer(d):
        return at(y * NZ_ + lax.rem(z + d, NZ_))

    def y_peer(d):
        return at(lax.rem(y + d, NY_) * NZ_ + z)

    def plane_peer(i):
        return at(lax.rem(y + i // NZ_, NY_) * NZ_ + lax.rem(z + i % NZ_, NZ_))

    loads = [
        pltpu.make_async_copy(src, dst, load_sem.at[i])
        for i, (src, dst) in enumerate(
            (
                (u0_hbm.at[other, :, 0], swap_out.at[pl.ds(2, 3)]),
                (u0_hbm.at[h, :, 0], u0_buf.at[h]),
                (dens_hbm, dens_ref),
                (des_hbm, des_ref),
                (sup_hbm, sup_ref),
                (nodes_hbm, nodes_ref),
                (forces_hbm, forces_ref),
            )
        )
    ]
    for copy in loads:
        copy.start()

    phases = contextlib.ExitStack()

    def mark(name):
        phases.close()
        if name:
            phases.enter_context(jax.named_scope(name))

    mark("signals")
    barrier = pltpu.get_barrier_semaphore()
    for d in range(1, RING):
        pl.semaphore_signal(barrier, inc=1, device_id=ring_peer(d)[1], device_id_type=MESH)
    for i in range(1, PLANE):
        pl.semaphore_signal(barrier, inc=1, device_id=plane_peer(i), device_id_type=MESH)

    sent = []

    def start(src, dst, ss, rs, device):
        copy = pltpu.make_async_remote_copy(
            src_ref=src, dst_ref=dst, send_sem=ss, recv_sem=rs,
            device_id=device, device_id_type=MESH,
        )
        copy.start()
        return copy

    def whole(ref, ss, rs):
        return pltpu.make_async_remote_copy(
            src_ref=ref, dst_ref=ref, send_sem=ss, recv_sem=rs,
            device_id=partner, device_id_type=MESH,
        )

    def one(slot, src, dst, device):
        copy = start(src, dst, one_send.at[slot], one_recv.at[slot], device)
        sent.append(copy)
        return copy

    def group(slot, buf, count, src, peer):
        for d in range(1, count):
            start(src(d), buf.at[d], group_send.at[slot], group_recv.at[slot], peer(d))
        rest = whole(buf.at[pl.ds(1, count - 1)], group_send.at[slot], group_recv.at[slot])
        sent.append(rest)
        return rest

    row = lax.broadcasted_iota(jnp.int32, (8, COLS), 0)
    col = lax.broadcasted_iota(jnp.int32, (8, COLS), 1)
    zero8 = jnp.zeros((8, COLS), F32)

    @pl.loop(0, NY_ * NZ_)
    def _(i):
        dy, dz = i // NZ_, lax.rem(i, NZ_)
        offset = 16 * (lax.rem(y + dy, NY_) - y) + 2 * (z - lax.rem(z + NZ_ - dz, NZ_))
        for a in range(3):
            t = jnp.full((8, COLS), offset + (a - 1), jnp.int32).astype(F32) * (1.0 / RADIUS)
            coef_buf[i * 3 + a] = jnp.exp(-(t * t))

    mark("prep")
    for step in range(SWEEPS + 1):
        for n in range(4):
            for c in range(3):
                t_buf[step, n, c, ROWS : ROWS + 8] = zero8
    for n in range(2):
        for c in range(3):
            tu_buf[n, c, ROWS : ROWS + 8] = zero8
    @pl.when(k == 0)
    def _():
        c_buf[0] = jnp.zeros((ROWS, COLS), F32)
        for step in range(SWEEPS):
            t_buf[step, 0, :, 0:ROWS] = jnp.zeros((3, ROWS, COLS), F32)

    @pl.when(k == PLANE - 1)
    def _():
        for step in range(SWEEPS + 1):
            t_buf[step, 3, :, 0:ROWS] = jnp.zeros((3, ROWS, COLS), F32)

    for copy in loads:
        copy.wait()
    dens = dens_ref[0]
    solid = des_ref[0].astype(F32) * dens
    cube = solid * solid * solid
    free_own = 1.0 - sup_ref[0].astype(F32)
    c_buf[1 + h] = cube
    free_buf[h] = free_own
    solid_buf[h] = solid
    swap_out[0] = solid
    swap_out[1] = free_own
    for c in range(3):
        t_buf[0, 1 + h, c, 0:ROWS] = u0_buf[h, c] * free_own
    mark("barrier")
    pl.semaphore_wait(barrier, RING - 1 + PLANE - 1)

    mark("sends0")
    toward = jnp.where(h == 0, below, above)
    away = jnp.where(h == 0, above, below)

    inside = jnp.logical_and(k > 0, k < PLANE - 1)

    def piece(p):
        if isinstance(p, int):
            return pl.ds(8 * p, 8) if p < 2 else pl.ds(16 * p - 16, 16)
        return pl.ds(pl.multiple_of(16 * p - 16, 16), 16)

    def each_piece(do):
        do(0)
        do(1)
        pl.loop(2, PIECES)(do)

    for p in range(PIECES):
        start(
            swap_out.at[:, piece(p)], swap_in.at[:, piece(p)],
            one_send.at[0], swap_recv.at[p], partner,
        )
    sent.append(whole(swap_out, one_send.at[0], swap_recv.at[0]))

    @pl.when(jnp.where(h == 0, k > 0, k < PLANE - 1))
    def _():
        for p in range(PIECES):
            start(
                t_buf.at[0, 1 + h, :, piece(p)], t_buf.at[0, 3 * other, :, piece(p)],
                halo_send.at[0], halo_recv.at[0, p], at(toward),
            )

    mark("smooth")
    gauss_x, gauss_y = gauss(ROWS), gauss(COLS)
    smooth_buf[...] = dot(dot(gauss_x, dens), gauss_y)
    mine8 = pl.ds(pl.multiple_of(8 * j, 8), 8)
    other8 = pl.ds(pl.multiple_of(8 * (other * LOADS_AX + l), 8), 8)
    fz_buf[0, 0, h] = smooth_buf[mine8]
    row_out[...] = smooth_buf[other8]
    got_rows = one(1, row_out, row_in, partner)

    mark("rhs")
    base = k * (2 * ROWS)
    line = lax.broadcasted_iota(jnp.int32, (2 * ROWS, CHUNK), 0)
    for n in range(2):
        for c in range(3):
            rhs_buf[n, c] = jnp.zeros((ROWS, COLS), F32)

    @pl.loop(0, POINTS // CHUNK)
    def _(i):
        cut = pl.ds(pl.multiple_of(i * CHUNK, CHUNK), CHUNK)
        node = jnp.where(h == 0, nodes_ref[0:1, cut], nodes_ref[1:2, cut])
        place = jnp.where((node >> 7) - base == line, 1.0, 0.0).astype(jnp.bfloat16)
        across = (node & 127) == line
        for c in range(3):
            force = jnp.where(h == 0, forces_ref[c, 0:1, cut], forces_ref[c, 1:2, cut])
            spread = jnp.where(across, force, 0.0)
            total = jnp.zeros((2 * ROWS, COLS), F32)
            for part in range(3):
                bits = spread.astype(jnp.bfloat16)
                total = total + lax.dot_general(
                    place, bits, (((1,), (1,)), ((), ())), preferred_element_type=F32
                )
                if part < 2:
                    spread = spread - bits.astype(F32)
            rhs_buf[0, c] += total[:ROWS]
            rhs_buf[1, c] += total[ROWS:]

    def z_send(slot, which):
        return group(slot, fz_buf.at[which], NZ_, lambda d: fz_buf.at[which, 0], z_peer)

    def z_mix(which):
        @pl.loop(0, NY_)
        def _(dy):
            for a in range(2):
                total = None
                for d in range(NZ_):
                    for b in range(2):
                        term = coef_buf[dy * (3 * NZ_) + (3 * d + a - b + 1)] * fz_buf[which, d, b]
                        total = term if total is None else total + term
                ps_buf[which, dy, a] = total

        for a in range(2):
            fy_buf[which, 0, a] = ps_buf[which, 0, a]

    def y_send(slot, which):
        return group(slot, fy_buf.at[which], NY_, lambda d: ps_buf.at[which, d], y_peer)

    def y_sum(which):
        return [
            fy_buf[which, 0, a] + fy_buf[which, 1, a] + fy_buf[which, 2, a] + fy_buf[which, 3, a]
            for a in range(2)
        ]

    def sum_of(buf, count):
        tile = buf[0]
        for d in range(1, count):
            tile = tile + buf[d]
        return tile

    mark("rows")
    got_rows.wait_recv()
    fz_buf[0, 0, other] = row_in[...]
    zs = z_send(0, 0)

    mark("forward")

    has_away = jnp.where(h == 0, k < PLANE - 1, k > 0)

    def forward(p):
        rows = piece(p)
        whole(swap_in.at[:, rows], one_send.at[0], swap_recv.at[p]).wait_recv()
        free = swap_in[1, rows]
        free_buf[other, rows] = free
        part = swap_in[0, rows]
        solid_buf[other, rows] = part
        c_buf[1 + other, rows] = part * part * part
        for c in range(3):
            u = swap_in[2 + c, rows]
            u0_buf[other, c, rows] = u
            t_buf[0, 1 + other, c, rows] = u * free

        @pl.when(has_away)
        def _():
            start(
                t_buf.at[0, 1 + other, :, rows], t_buf.at[0, 3 * h, :, rows],
                halo_send.at[0], halo_recv.at[0, p], at(away),
            )

        @pl.when(k < PLANE - 1)
        def _():
            start(c_buf.at[2, rows], c_buf.at[0, rows], one_send.at[2], c_recv.at[p], at(above))

    each_piece(forward)
    has_below = jnp.where(k > 0, 1.0, 0.0)
    def wait_piece(step, p):
        rows = piece(p)
        if step == 0:
            @pl.when(k > 0)
            def _():
                whole(c_buf.at[0, rows], one_send.at[2], c_recv.at[p]).wait_recv()

        @pl.when(inside)
        def _():
            whole(
                t_buf.at[step, 1:3, :, rows], halo_send.at[step], halo_recv.at[step, p]
            ).wait_recv()

        @pl.when(jnp.logical_not(inside))
        def _():
            whole(
                t_buf.at[step, 1, :, rows], halo_send.at[step], halo_recv.at[step, p]
            ).wait_recv()

    def chunk_rows(i):
        return pl.ds(8 * i, 8) if isinstance(i, int) else pl.ds(pl.multiple_of(i * 8, 8), 8)

    def operate(step, before, finish, extra, meanwhile=None):
        def chunk(i, behind, extra):
            behind = list(behind)
            rows, after = chunk_rows(i), chunk_rows(i + 1)
            stiff, extra = before(rows, extra)
            total = [None, None]
            lower = None
            for n in range(4):
                upper = []
                for c in range(3):
                    v, w = t_buf[step, n, c, rows], t_buf[step, n, c, after]
                    upper.append(plane_modes(v, w, row, col))
                if n:
                    e = n - 1
                    f = cell_forces(cell_modes(lower, upper), stiff[e])
                    for node, sign in ((e, 1.0), (e - 1, -1.0)):
                        if not 0 <= node < 2:
                            continue
                        part = {}
                        for c in range(3):
                            for q in range(4):
                                hi = f[4 + q, c]
                                if q == 0:
                                    value = hi if sign > 0 else -hi
                                else:
                                    value = f[q, c] + hi if sign > 0 else f[q, c] - hi
                                part[c, q] = value
                        if total[node] is None:
                            total[node] = part
                        else:
                            total[node] = {key: total[node][key] + part[key] for key in part}
                lower = upper
            for node in range(2):
                for c in range(3):
                    g = []
                    for px in range(2):
                        fs, fd = total[node][c, 2 * px], total[node][c, 2 * px + 1]
                        shifted = jnp.where(col == 0, 0.0, pltpu.roll(fs + fd, 1, 1))
                        g.append(fs - fd + shifted)
                    r = pltpu.roll(g[0] + g[1], 1, 0)
                    slot = 3 * node + c
                    value = g[0] - g[1] + jnp.where(row == 0, behind[slot], r)
                    behind[slot] = r
                    extra = finish(node, c, rows, value, extra)
            return tuple(behind), extra

        def body(p, carry):
            behind, extra = carry

            @pl.when(p < PIECES - 1)
            def _():
                wait_piece(step, p + 1)

            for part in range(2):
                behind, extra = chunk(2 * p - 2 + part, behind, extra)
            send_piece(step + 1, p)
            return behind, extra

        mark(f"wait{step}")
        wait_piece(step, 0)
        if meanwhile:
            meanwhile()
        mark(f"app{step}")
        behind = (zero8,) * 6
        for p in range(2):
            wait_piece(step, p + 1)
            behind, extra = chunk(p, behind, extra)
            send_piece(step + 1, p)
        return lax.fori_loop(2, PIECES, body, (behind, extra))[1]

    def send_piece(step, p):
        rows = piece(p)
        if step < SWEEPS:
            @pl.when(k < PLANE - 1)
            def _():
                start(
                    t_buf.at[step, 2, :, rows], t_buf.at[step, 0, :, rows],
                    halo_send.at[step], halo_recv.at[step, p], at(above),
                )

        @pl.when(k > 0)
        def _():
            start(
                t_buf.at[step, 1, :, rows], t_buf.at[step, 3, :, rows],
                halo_send.at[step], halo_recv.at[step, p], at(below),
            )

    def stiffness(rows, extra):
        acc, rolls = extra
        stiff = [STIFF_VOID + (1.0 - STIFF_VOID) * c_buf[e, rows] for e in range(3)]
        stiff[0] = stiff[0] * has_below
        out = []
        for e in range(3):
            stiff_buf[e, rows] = stiff[e]
        for n in range(2):
            b = stiff[n] + stiff[n + 1]
            b = b + jnp.where(col == 0, 0.0, pltpu.roll(b, 1, 1))
            r = pltpu.roll(b, 1, 0)
            b = b + jnp.where(row == 0, rolls[n], r)
            out.append(r)
            free = free_buf[n, rows]
            inv_buf[n, rows] = 1.0 / (free * KD * b + (1.0 - free))
        return stiff, (acc, tuple(out))

    def first(n, c, rows, value, extra):
        free, inv = free_buf[n, rows], inv_buf[n, rows]
        r = free * (rhs_buf[n, c, rows] - value) - (1.0 - free) * u0_buf[n, c, rows]
        g = r * inv
        v_buf[0, n, c, rows] = g
        t_buf[1, 1 + n, c, rows] = free * g
        return extra[0] + r * g, extra[1]

    def held(rows, extra):
        return [stiff_buf[e, rows] for e in range(3)], extra

    def later(step):
        def finish(n, c, rows, value, extra):
            free, inv = free_buf[n, rows], inv_buf[n, rows]
            v = v_buf[step - 1, n, c, rows]
            w = free * value + (1.0 - free) * v
            new = w * inv
            v_buf[step, n, c, rows] = new
            t_buf[step + 1, 1 + n, c, rows] = free * new
            return extra + v * w if step == 1 else extra

        return finish

    gr = operate(0, stiffness, first, (zero8, (zero8, zero8)))[0]
    mark("mid0")
    zs.wait_recv()
    z_mix(0)
    ys = y_send(1, 0)
    count8 = zero8
    for n in range(2):
        for i in range(ROWS // 8):
            count8 = count8 + jnp.where(solid_buf[n, 8 * i : 8 * i + 8] > 0.0, 1.0, 0.0)
    gw = operate(1, held, later(1), zero8)

    mark("mid1")
    lane = lax.broadcasted_iota(jnp.int32, (1, COLS), 1)
    line0 = jnp.zeros((1, COLS), F32)
    for i, tile in enumerate((gr, gw, count8)):
        line0 = jnp.where(lane == i, total_of(tile), line0)
    sz_buf[0] = line0
    scalars = group(2, sz_buf, PLANE, lambda i: sz_buf.at[0], plane_peer)
    ys.wait_recv()
    denom = y_sum(0)
    for a in range(2):
        den_buf[a] = denom[a]
        fz_buf[1, 0, a] = jnp.where(solid_buf[a, mine8] > 0.0, 1.0, 0.0) / denom[a]
    zs = z_send(3, 1)
    operate(2, held, later(2), 0)
    q_flight = []

    def q_mix():
        zs.wait_recv()
        z_mix(1)
        q_flight.append(y_send(5, 1))

    operate(3, held, later(3), 0, q_mix)
    mark("combine")
    scalars.wait_recv()
    line0 = sum_of(sz_buf, PLANE)
    gr_all, gw_all, count = line0[:, 0:1], line0[:, 1:2], line0[:, 2:3]
    coefs = [jnp.broadcast_to(c, (8, COLS)) for c in chebyshev(UPPER_FACTOR * gw_all / gr_all)]

    @pl.loop(0, ROWS // 8)
    def _(i):
        rows = pl.ds(pl.multiple_of(i * 8, 8), 8)
        for n in range(2):
            free = free_buf[n, rows]
            for c in range(3):
                u = u0_buf[n, c, rows]
                for power in range(SWEEPS):
                    u = u + coefs[power] * v_buf[power, n, c, rows]
                send_buf[n, c, rows] = u
                tu_buf[n, c, rows] = free * u

    def own_layer(n, c, rows):
        return tu_buf[n, c, rows]

    def upper_layer(n, c, rows):
        if n < 2:
            return tu_buf[n, c, rows]
        u = t_buf[0, 3, c, rows]
        for power in range(SWEEPS):
            u = u + coefs[power] * t_buf[power + 1, 3, c, rows]
        return u

    def energy_chunk(e, layer, i):
        rows, after = chunk_rows(i), chunk_rows(i + 1)
        planes = [
            [plane_modes(layer(n, c, rows), layer(n, c, after), row, col) for c in range(3)]
            for n in (e, e + 1)
        ]
        value = cell_energy(cell_modes(*planes))
        weight = (3.0 * (1.0 - STIFF_VOID)) * c_buf[1 + e, rows]
        num_buf[e, rows] = weight * value

    def smooth_xy(plane):
        return dot(gauss_x, dot(plane, gauss_y))

    mark("energy0")

    @pl.loop(0, ROWS // 16)
    def _(p):
        for part in range(2):
            energy_chunk(0, own_layer, 2 * p + part)

    rs0 = smooth_xy(num_buf[0])
    mark("wait_last")

    def last_piece(p):
        @pl.when(k < PLANE - 1)
        def _():
            whole(
                t_buf.at[SWEEPS, 3, :, piece(p)], halo_send.at[SWEEPS], halo_recv.at[SWEEPS, p]
            ).wait_recv()

    last_piece(0)
    for p in range(2):
        last_piece(p + 1)
        energy_chunk(1, upper_layer, p)

    @pl.loop(2, PIECES)
    def _(p):
        @pl.when(p < PIECES - 1)
        def _():
            last_piece(p + 1)

        for part in range(2):
            energy_chunk(1, upper_layer, 2 * p - 2 + part)

    mark("smoothn")
    rs1 = smooth_xy(num_buf[1])
    num2_buf[0] = rs0
    num2_buf[1] = rs1
    for a in range(2):
        rs_buf[0, a] = num2_buf[a, mine8]
    xs = group(
        7, rs_buf, RING,
        lambda d: num2_buf.at[:, pl.ds(pl.multiple_of(8 * ring_peer(d)[0], 8), 8)],
        lambda d: ring_peer(d)[1],
    )
    mark("wait_rs")
    xs.wait_recv()
    totals = [sum_of(rs_buf.at[:, a], RING) for a in range(2)]
    for a in range(2):
        fz_buf[2, 0, a] = totals[a]
    zs = z_send(4, 2)
    mark("wpart")
    q_flight[0].wait_recv()
    q8 = y_sum(1)
    wx_buf[0] = jnp.sum(q8[0] * totals[0] + q8[1] * totals[1], axis=0, keepdims=True)
    wxs = group(8, wx_buf, RING, lambda d: wx_buf.at[0], lambda d: ring_peer(d)[1])
    got_back = one(3, send_buf.at[other], back_buf, partner)
    for c in range(3):
        disp_out[h, c, 0] = send_buf[h, c]
    mark("wait_wx")
    wxs.wait_recv()
    wz_buf[0] = sum_of(wx_buf, RING)
    wzs = group(9, wz_buf, PLANE, lambda i: wz_buf.at[0], plane_peer)
    mark("wait_z")
    zs.wait_recv()
    mark("zmix2")
    z_mix(2)
    ys = y_send(6, 2)
    mark("wait_y")
    ys.wait_recv()
    numer = y_sum(2)
    for a in range(2):
        here = jnp.where(solid_buf[a, mine8] > 0.0, 1.0, 0.0)
        xt_buf[0, a] = here * (numer[a] / den_buf[a])
    xs = group(10, xt_buf, RING, lambda d: xt_buf.at[0], lambda d: ring_peer(d)[1])
    mark("wait_wz")
    wzs.wait_recv()
    weighted_all = jnp.sum(sum_of(wz_buf, PLANE), axis=1, keepdims=True)
    inv_mean = 1.0 / (weighted_all / count + EPSILON)
    mark("wait_x")
    xs.wait_recv()
    mark("trial")
    tile = zero8
    for d in range(RING):
        there = pl.ds(pl.multiple_of(8 * lax.rem(j + RING - d, RING), 8), 8)
        for a in range(2):
            old = solid_buf[a, there]
            trial = jnp.minimum(
                jnp.maximum(old * jnp.sqrt(xt_buf[d, a] * inv_mean), old - MOVE_LIMIT),
                old + MOVE_LIMIT,
            )
            tile = tile + trial
            trial_buf[a, there] = trial
    vol_buf[0] = jnp.sum(tile, axis=0, keepdims=True)
    vs = group(11, vol_buf, PLANE, lambda i: vol_buf.at[0], plane_peer)
    mark("wait_back")
    got_back.wait_recv()
    for c in range(3):
        disp_out[other, c, 0] = back_buf[c]
    for copy in sent[:-1]:
        copy.wait_send()

    def layers_sent(step, layers):
        whole(
            t_buf.at[step, layers, :, 0:ROWS], halo_send.at[step], halo_recv.at[step, 0]
        ).wait_send()

    for step in range(SWEEPS):
        pl.when(inside)(lambda: layers_sent(step, pl.ds(1, 2)))
        pl.when(jnp.logical_not(inside))(lambda: layers_sent(step, 1))
    pl.when(k > 0)(lambda: layers_sent(SWEEPS, 1))
    pl.when(k < PLANE - 1)(lambda: whole(c_buf.at[0], one_send.at[2], c_recv.at[0]).wait_send())
    mark("wait_vol")
    vs.wait_recv()
    mark("finish")
    volume = jnp.sum(sum_of(vol_buf, PLANE), axis=1, keepdims=True)
    scale = VOLUME_TARGET / (volume / count + EPSILON)
    dens_out[0] = jnp.minimum(scale * trial_buf[h], 1.0)
    vs.wait_send()
    mark(None)


def shards(start_disp, density, design, support, load_nodes, load_forces):
    arrays = (
        start_disp, density, design, support, load_nodes, jnp.transpose(load_forces, (1, 0, 2)),
    )
    vmem = lambda *shape: pltpu.VMEM(shape, F32)
    dma = lambda *shape: pltpu.SemaphoreType.DMA(shape)
    plane = (ROWS, COLS)
    return pl.pallas_call(
        kernel,
        out_shape=(
            pltpu.VMEM(start_disp.shape, F32),
            pltpu.VMEM(density.shape, F32),
        ),
        in_specs=[pl.BlockSpec(memory_space=pltpu.HBM)] * 6,
        out_specs=(pl.BlockSpec(memory_space=pltpu.VMEM),) * 2,
        scratch_shapes=[
            vmem(1, *plane),
            pltpu.VMEM((1, *plane), jnp.int32),
            pltpu.VMEM((1, *plane), jnp.int32),
            pltpu.VMEM((2, POINTS), jnp.int32),
            vmem(3, 2, POINTS),
            vmem(SWEEPS + 1, 4, 3, ROWS + 8, COLS),
            vmem(SWEEPS, 2, 3, *plane),
            vmem(2, 3, *plane),
            vmem(2, 3, *plane),
            vmem(3, *plane),
            vmem(2, *plane),
            vmem(3, *plane),
            vmem(2, *plane),
            vmem(2, *plane),
            vmem(5, *plane),
            vmem(5, *plane),
            vmem(2, 3, ROWS + 8, COLS),
            vmem(2, 3, *plane),
            vmem(3, *plane),
            vmem(3 * NY_ * NZ_, 8, COLS),
            vmem(8, COLS),
            vmem(8, COLS),
            vmem(3, NZ_, 2, 8, COLS),
            vmem(3, NY_, 2, 8, COLS),
            vmem(3, NY_, 2, 8, COLS),
            vmem(*plane),
            vmem(2, *plane),
            vmem(2, *plane),
            vmem(RING, 2, 8, COLS),
            vmem(RING, 2, 8, COLS),
            vmem(2, *plane),
            vmem(2, 8, COLS),
            vmem(PLANE, 1, COLS),
            vmem(RING, 1, COLS),
            vmem(PLANE, 1, COLS),
            vmem(PLANE, 1, COLS),
            dma(7), dma(PIECES), dma(SWEEPS + 1, PIECES), dma(PIECES), dma(SWEEPS + 1),
            dma(4), dma(4), dma(12), dma(12),
        ],
        compiler_params=pltpu.CompilerParams(
            collective_id=0, has_side_effects=True, vmem_limit_bytes=48 * 1024 * 1024
        ),
    )(*(pltpu.with_memory_space_constraint(a, pltpu.HBM) for a in arrays))


def solution(mesh):
    return jax.shard_map(
        shards,
        mesh=mesh,
        in_specs=(
            P("load", None, "slab", None, None),
            P("slab", None, None),
            P("slab", None, None),
            P("slab", None, None),
            P("load", None),
            P("load", None, None),
        ),
        out_specs=(P("load", None, "slab", None, None), P("slab", None, None)),
        check_vma=False,
    )
```

```python
import contextlib

import jax
import jax.numpy as jnp
import numpy as np
from jax import lax
from jax.experimental import pallas as pl
from jax.experimental.pallas import tpu as pltpu
from jax.sharding import PartitionSpec as P

SWEEPS = 4
RADIUS = 2
POISSON = 0.3
STIFF_VOID = 0.001
UPPER_FACTOR = 1.2
LOWER_RATIO = 0.1
MOVE_LIMIT = 0.2
VOLUME_TARGET = 0.5
EPSILON = 1e-06
HIGHEST = lax.Precision.HIGHEST
MESH = pl.DeviceIdType.MESH
F32 = jnp.float32

NY_, NZ_ = 4, 8
LOADS_AX = 4
RING = 2 * LOADS_AX
PLANE = NY_ * NZ_
ROWS, COLS = 64, 128
POINTS = 2048
CHUNK = 256
PIECES = 5


def hex_stiffness():
    lame_first = POISSON / ((1 + POISSON) * (1 - 2 * POISSON))
    lame_shear = 1 / (2 * (1 + POISSON))
    elastic = np.zeros((6, 6))
    elastic[:3, :3] = lame_first
    for axis_a in range(3):
        elastic[axis_a, axis_a] += 2 * lame_shear
        elastic[3 + axis_a, 3 + axis_a] = lame_shear
    shear_pairs = ((0, 1), (1, 2), (0, 2))
    gauss_point = 1 / np.sqrt(3)
    matrix = np.zeros((24, 24))
    for quad_index in range(8):
        quad_coords = [
            gauss_point * (2 * (quad_index >> 2 - axis_a & 1) - 1) for axis_a in range(3)
        ]
        shape_grads = np.zeros((8, 3))
        for corner in range(8):
            corner_signs = [2 * (corner >> 2 - axis_a & 1) - 1 for axis_a in range(3)]
            for axis_a in range(3):
                deriv_value = float(corner_signs[axis_a])
                for axis_b in range(3):
                    if axis_b != axis_a:
                        deriv_value *= (1 + corner_signs[axis_b] * quad_coords[axis_b]) / 2
                shape_grads[corner, axis_a] = deriv_value
        strain = np.zeros((6, 24))
        for corner in range(8):
            for axis_a in range(3):
                strain[axis_a, 3 * corner + axis_a] = shape_grads[corner, axis_a]
            for pair_index, shear_pair in enumerate(shear_pairs):
                strain[3 + pair_index, 3 * corner + shear_pair[0]] = shape_grads[
                    corner, shear_pair[1]
                ]
                strain[3 + pair_index, 3 * corner + shear_pair[1]] = shape_grads[
                    corner, shear_pair[0]
                ]
        matrix += strain.T @ elastic @ strain / 8
    return matrix.astype(np.float32)


def mode_stiffness():
    ke = hex_stiffness().astype(np.float64)
    w = np.zeros((24, 24))
    for p in range(8):
        for o in range(8):
            sign = 1.0
            for a in range(3):
                if p >> (2 - a) & 1:
                    sign *= 1.0 if o >> (2 - a) & 1 else -1.0
            for c in range(3):
                w[3 * p + c, 3 * o + c] = sign
    return w @ ke @ w.T / 64


KHAT = mode_stiffness()
KD = float(hex_stiffness()[0, 0])


def kh(p, c, q, d):
    return float(KHAT[3 * p + c, 3 * q + d])


SHEAR = kh(1, 0, 1, 0)
TRACE = kh(1, 2, 2, 1)
NORMAL = kh(1, 2, 1, 2) - TRACE
TWIST = kh(3, 0, 5, 1)
BEND = kh(3, 1, 3, 1)
CROSS = kh(3, 1, 5, 0)
LAST = kh(7, 0, 7, 0)

SHEAR_PAIRS = (((1, 0), (4, 2)), ((1, 1), (2, 2)), ((2, 0), (4, 1)))
NORMALS = ((4, 0), (2, 1), (1, 2))
TWISTS = ((3, 0), (5, 1), (6, 2))
BENDS = (((3, 1), (5, 0)), ((3, 2), (6, 0)), ((5, 2), (6, 1)))


def check_table():
    table = np.zeros((24, 24))

    def put(a, b, v):
        table[3 * a[0] + a[1], 3 * b[0] + b[1]] = v

    for a, b in SHEAR_PAIRS:
        for u in (a, b):
            for v in (a, b):
                put(u, v, SHEAR)
    for a in NORMALS:
        for b in NORMALS:
            put(a, b, TRACE + (NORMAL if a == b else 0))
    for a in TWISTS:
        for b in TWISTS:
            put(a, b, 2 * TWIST if a == b else TWIST)
    for a, b in BENDS:
        put(a, a, BEND)
        put(b, b, BEND)
        put(a, b, CROSS)
        put(b, a, CROSS)
    for c in range(3):
        put((7, c), (7, c), LAST)
    assert np.abs(table - KHAT).max() < 1e-8


check_table()


def shift_rows_up(v, after, row):
    return pltpu.roll(jnp.where(row == 0, after, v), 7, 0)


def plane_modes(v, after, row, col):
    ahead = shift_rows_up(v, after, row)
    out = {}
    for px, f in ((0, v + ahead), (1, ahead - v)):
        fa = jnp.where(col == COLS - 1, 0.0, pltpu.roll(f, COLS - 1, 1))
        out[px, 0] = f + fa
        out[px, 1] = fa - f
    return out


def cell_modes(bottom, top):
    m = {}
    for c in range(3):
        for p in range(1, 8):
            xy = (p >> 1 & 1, p & 1)
            b, t = bottom[c][xy], top[c][xy]
            m[p, c] = t - b if p >> 2 else t + b
    return m


def cell_forces(m, stiff):
    f = {}
    shear, trace, normal = stiff * SHEAR, stiff * TRACE, stiff * NORMAL
    twist, bend, cross, last = stiff * TWIST, stiff * BEND, stiff * CROSS, stiff * LAST
    for a, b in SHEAR_PAIRS:
        f[a] = f[b] = shear * (m[a] + m[b])
    total = trace * (m[NORMALS[0]] + m[NORMALS[1]] + m[NORMALS[2]])
    for a in NORMALS:
        f[a] = total + normal * m[a]
    total = m[TWISTS[0]] + m[TWISTS[1]] + m[TWISTS[2]]
    for a in TWISTS:
        f[a] = twist * (total + m[a])
    for a, b in BENDS:
        f[a] = bend * m[a] + cross * m[b]
        f[b] = cross * m[a] + bend * m[b]
    for c in range(3):
        f[7, c] = last * m[7, c]
    return f


def cell_energy(m):
    shear = None
    for a, b in SHEAR_PAIRS:
        s = m[a] + m[b]
        shear = s * s if shear is None else shear + s * s
    total = m[NORMALS[0]] + m[NORMALS[1]] + m[NORMALS[2]]
    normal = m[NORMALS[0]] * m[NORMALS[0]] + m[NORMALS[1]] * m[NORMALS[1]] + m[NORMALS[2]] * m[NORMALS[2]]
    twist = m[TWISTS[0]] + m[TWISTS[1]] + m[TWISTS[2]]
    twists = twist * twist
    for a in TWISTS:
        twists = twists + m[a] * m[a]
    bends = None
    crosses = None
    for a, b in BENDS:
        s = m[a] * m[a] + m[b] * m[b]
        t = m[a] * m[b]
        bends = s if bends is None else bends + s
        crosses = t if crosses is None else crosses + t
    last = m[7, 0] * m[7, 0] + m[7, 1] * m[7, 1] + m[7, 2] * m[7, 2]
    return (
        SHEAR * shear
        + TRACE * (total * total)
        + NORMAL * normal
        + TWIST * twists
        + BEND * bends
        + (2.0 * CROSS) * crosses
        + LAST * last
    )


def gauss(count):
    t = (
        lax.broadcasted_iota(jnp.int32, (count, count), 0)
        - lax.broadcasted_iota(jnp.int32, (count, count), 1)
    ).astype(F32) * (1.0 / RADIUS)
    return jnp.exp(-(t * t))


def dot(a, b):
    return lax.dot_general(
        a, b, (((1,), (0,)), ((), ())), precision=HIGHEST, preferred_element_type=F32
    )


def total_of(tile):
    return jnp.sum(jnp.sum(tile, axis=0, keepdims=True), axis=1, keepdims=True)


def chebyshev(upper):
    lower = LOWER_RATIO * upper
    center = 0.5 * (upper + lower)
    half_width = 0.5 * (upper - lower)
    spread = center / half_width
    factor = 1.0 / spread
    zero = jnp.zeros_like(upper)
    e = [jnp.ones_like(upper)] + [zero] * (SWEEPS - 1)
    d = [1.0 / center] + [zero] * (SWEEPS - 1)
    u = [zero] * SWEEPS
    for sweep in range(SWEEPS):
        u = [a + b for a, b in zip(u, d)]
        if sweep < SWEEPS - 1:
            e = [e[0]] + [e[n] - d[n - 1] for n in range(1, SWEEPS)]
            after = 1.0 / (2.0 * spread - factor)
            d = [after * factor * a + 2.0 * after / half_width * b for a, b in zip(d, e)]
            factor = after
    return u


def kernel(
    u0_hbm, dens_hbm, des_hbm, sup_hbm, nodes_hbm, forces_hbm,
    disp_out, dens_out,
    dens_ref, des_ref, sup_ref, nodes_ref, forces_ref,
    t_buf, v_buf, u0_buf, rhs_buf, c_buf, solid_buf, stiff_buf, inv_buf, free_buf,
    swap_out, swap_in, tu_buf, send_buf, back_buf, coef_buf, row_out, row_in,
    fz_buf, ps_buf, fy_buf, smooth_buf, num_buf, num2_buf, rs_buf, xt_buf, trial_buf,
    den_buf, sz_buf, wx_buf, wz_buf, vol_buf,
    heard, load_sem, swap_recv, halo_recv, c_recv, halo_send, one_send, one_recv, group_send, group_recv,
):
    s = lax.axis_index("slab")
    l = lax.axis_index("load")
    h = lax.rem(s, 2)
    k = s // 2
    z = lax.rem(k, NZ_)
    y = k // NZ_
    j = h * LOADS_AX + l
    other = 1 - h

    def at(group, half=None, load=None):
        return {
            "slab": group * 2 + (h if half is None else half),
            "load": l if load is None else load,
        }

    above = lax.rem(k + 1, PLANE)
    below = lax.rem(k + PLANE - 1, PLANE)
    partner = at(k, half=other)

    def ring_peer(d):
        t = lax.rem(j + d, RING)
        return t, at(k, half=t // LOADS_AX, load=lax.rem(t, LOADS_AX))

    def z_peer(d):
        return at(y * NZ_ + lax.rem(z + d, NZ_))

    def y_peer(d):
        return at(lax.rem(y + d, NY_) * NZ_ + z)

    def plane_peer(i):
        return at(lax.rem(y + i // NZ_, NY_) * NZ_ + lax.rem(z + i % NZ_, NZ_))

    loads = [
        pltpu.make_async_copy(src, dst, load_sem.at[i])
        for i, (src, dst) in enumerate(
            (
                (u0_hbm.at[other, :, 0], swap_out.at[pl.ds(2, 3)]),
                (u0_hbm.at[h, :, 0], u0_buf.at[h]),
                (dens_hbm, dens_ref),
                (des_hbm, des_ref),
                (sup_hbm, sup_ref),
                (nodes_hbm, nodes_ref),
                (forces_hbm, forces_ref),
            )
        )
    ]
    for copy in loads:
        copy.start()

    phases = contextlib.ExitStack()

    def mark(name):
        phases.close()
        if name:
            phases.enter_context(jax.named_scope(name))

    mark("signals")
    barrier = pltpu.get_barrier_semaphore()
    near = [ring_peer(d)[1] for d in range(1, RING)]
    near += [y_peer(d) for d in range(1, NY_)]
    near += [z_peer(d) for d in (1, 2, NZ_ - 2, NZ_ - 1)]
    near += [at(above), at(below)]
    for device in near:
        pl.semaphore_signal(barrier, inc=1, device_id=device, device_id_type=MESH)

    sent = []

    def start(src, dst, ss, rs, device):
        copy = pltpu.make_async_remote_copy(
            src_ref=src, dst_ref=dst, send_sem=ss, recv_sem=rs,
            device_id=device, device_id_type=MESH,
        )
        copy.start()
        return copy

    def whole(ref, ss, rs):
        return pltpu.make_async_remote_copy(
            src_ref=ref, dst_ref=ref, send_sem=ss, recv_sem=rs,
            device_id=partner, device_id_type=MESH,
        )

    def one(slot, src, dst, device):
        copy = start(src, dst, one_send.at[slot], one_recv.at[slot], device)
        sent.append(copy)
        return copy

    def group(slot, buf, count, src, peer):
        for d in range(1, count):
            start(src(d), buf.at[d], group_send.at[slot], group_recv.at[slot], peer(d))
        rest = whole(buf.at[pl.ds(1, count - 1)], group_send.at[slot], group_recv.at[slot])
        sent.append(rest)
        return rest

    row = lax.broadcasted_iota(jnp.int32, (8, COLS), 0)
    col = lax.broadcasted_iota(jnp.int32, (8, COLS), 1)
    zero8 = jnp.zeros((8, COLS), F32)

    mark("prep")
    for step in range(SWEEPS + 1):
        for n in range(4):
            for c in range(3):
                t_buf[step, n, c, ROWS : ROWS + 8] = zero8
    for n in range(2):
        for c in range(3):
            tu_buf[n, c, ROWS : ROWS + 8] = zero8
    @pl.when(k == 0)
    def _():
        c_buf[0] = jnp.zeros((ROWS, COLS), F32)
        for step in range(SWEEPS):
            t_buf[step, 0, :, 0:ROWS] = jnp.zeros((3, ROWS, COLS), F32)

    @pl.when(k == PLANE - 1)
    def _():
        for step in range(SWEEPS + 1):
            t_buf[step, 3, :, 0:ROWS] = jnp.zeros((3, ROWS, COLS), F32)

    for copy in loads:
        copy.wait()
    dens = dens_ref[0]
    solid = des_ref[0].astype(F32) * dens
    cube = solid * solid * solid
    free_own = 1.0 - sup_ref[0].astype(F32)
    c_buf[1 + h] = cube
    free_buf[h] = free_own
    solid_buf[h] = solid
    swap_out[0] = solid
    swap_out[1] = free_own
    for c in range(3):
        t_buf[0, 1 + h, c, 0:ROWS] = u0_buf[h, c] * free_own
    mark("barrier")
    pl.semaphore_wait(barrier, len(near))
    for d in (2, NZ_ - 2):
        pl.semaphore_signal(heard.at[0], inc=1, device_id=z_peer(d), device_id_type=MESH)

    mark("sends0")
    toward = jnp.where(h == 0, below, above)
    away = jnp.where(h == 0, above, below)

    inside = jnp.logical_and(k > 0, k < PLANE - 1)

    def piece(p):
        if isinstance(p, int):
            return pl.ds(8 * p, 8) if p < 2 else pl.ds(16 * p - 16, 16)
        return pl.ds(pl.multiple_of(16 * p - 16, 16), 16)

    def each_piece(do):
        do(0)
        do(1)
        pl.loop(2, PIECES)(do)

    for p in range(PIECES):
        start(
            swap_out.at[:, piece(p)], swap_in.at[:, piece(p)],
            one_send.at[0], swap_recv.at[p], partner,
        )
    sent.append(whole(swap_out, one_send.at[0], swap_recv.at[0]))

    @pl.when(jnp.where(h == 0, k > 0, k < PLANE - 1))
    def _():
        for p in range(PIECES):
            start(
                t_buf.at[0, 1 + h, :, piece(p)], t_buf.at[0, 3 * other, :, piece(p)],
                halo_send.at[0], halo_recv.at[0, p], at(toward),
            )

    mark("smooth")
    gauss_x, gauss_y = gauss(ROWS), gauss(COLS)
    smooth_buf[...] = dot(dot(gauss_x, dens), gauss_y)
    mine8 = pl.ds(pl.multiple_of(8 * j, 8), 8)
    other8 = pl.ds(pl.multiple_of(8 * (other * LOADS_AX + l), 8), 8)
    fz_buf[0, 0, h] = smooth_buf[mine8]
    row_out[...] = smooth_buf[other8]
    got_rows = one(1, row_out, row_in, partner)

    mark("coef")
    @pl.loop(0, NY_ * NZ_)
    def _(i):
        dy, dz = i // NZ_, lax.rem(i, NZ_)
        offset = 16 * (lax.rem(y + dy, NY_) - y) + 2 * (z - lax.rem(z + NZ_ - dz, NZ_))
        for a in range(3):
            t = jnp.full((8, COLS), offset + (a - 1), jnp.int32).astype(F32) * (1.0 / RADIUS)
            coef_buf[i * 3 + a] = jnp.exp(-(t * t))

    mark("rhs")
    base = k * (2 * ROWS)
    line = lax.broadcasted_iota(jnp.int32, (2 * ROWS, CHUNK), 0)
    for n in range(2):
        for c in range(3):
            rhs_buf[n, c] = jnp.zeros((ROWS, COLS), F32)

    @pl.loop(0, POINTS // CHUNK)
    def _(i):
        cut = pl.ds(pl.multiple_of(i * CHUNK, CHUNK), CHUNK)
        node = jnp.where(h == 0, nodes_ref[0:1, cut], nodes_ref[1:2, cut])
        place = jnp.where((node >> 7) - base == line, 1.0, 0.0).astype(jnp.bfloat16)
        across = (node & 127) == line
        for c in range(3):
            force = jnp.where(h == 0, forces_ref[c, 0:1, cut], forces_ref[c, 1:2, cut])
            spread = jnp.where(across, force, 0.0)
            total = jnp.zeros((2 * ROWS, COLS), F32)
            for part in range(3):
                bits = spread.astype(jnp.bfloat16)
                total = total + lax.dot_general(
                    place, bits, (((1,), (1,)), ((), ())), preferred_element_type=F32
                )
                if part < 2:
                    spread = spread - bits.astype(F32)
            rhs_buf[0, c] += total[:ROWS]
            rhs_buf[1, c] += total[ROWS:]

    def z_send(slot, which):
        return group(slot, fz_buf.at[which], NZ_, lambda d: fz_buf.at[which, 0], z_peer)

    def z_mix(which):
        @pl.loop(0, NY_)
        def _(dy):
            for a in range(2):
                total = None
                for d in range(NZ_):
                    for b in range(2):
                        term = coef_buf[dy * (3 * NZ_) + (3 * d + a - b + 1)] * fz_buf[which, d, b]
                        total = term if total is None else total + term
                ps_buf[which, dy, a] = total

        for a in range(2):
            fy_buf[which, 0, a] = ps_buf[which, 0, a]

    def y_send(slot, which):
        return group(slot, fy_buf.at[which], NY_, lambda d: ps_buf.at[which, d], y_peer)

    def y_sum(which):
        return [
            fy_buf[which, 0, a] + fy_buf[which, 1, a] + fy_buf[which, 2, a] + fy_buf[which, 3, a]
            for a in range(2)
        ]

    def sum_of(buf, count):
        tile = buf[0]
        for d in range(1, count):
            tile = tile + buf[d]
        return tile

    mark("rows")
    pl.semaphore_wait(heard.at[0], 2)
    for d in range(1, NY_):
        pl.semaphore_signal(heard.at[1], inc=1, device_id=y_peer(d), device_id_type=MESH)
    got_rows.wait_recv()
    fz_buf[0, 0, other] = row_in[...]
    zs = z_send(0, 0)

    mark("forward")

    has_away = jnp.where(h == 0, k < PLANE - 1, k > 0)

    def forward(p):
        rows = piece(p)
        whole(swap_in.at[:, rows], one_send.at[0], swap_recv.at[p]).wait_recv()
        free = swap_in[1, rows]
        free_buf[other, rows] = free
        part = swap_in[0, rows]
        solid_buf[other, rows] = part
        c_buf[1 + other, rows] = part * part * part
        for c in range(3):
            u = swap_in[2 + c, rows]
            u0_buf[other, c, rows] = u
            t_buf[0, 1 + other, c, rows] = u * free

        @pl.when(has_away)
        def _():
            start(
                t_buf.at[0, 1 + other, :, rows], t_buf.at[0, 3 * h, :, rows],
                halo_send.at[0], halo_recv.at[0, p], at(away),
            )

        @pl.when(k < PLANE - 1)
        def _():
            start(c_buf.at[2, rows], c_buf.at[0, rows], one_send.at[2], c_recv.at[p], at(above))

    each_piece(forward)
    has_below = jnp.where(k > 0, 1.0, 0.0)
    def wait_piece(step, p):
        rows = piece(p)
        if step == 0:
            @pl.when(k > 0)
            def _():
                whole(c_buf.at[0, rows], one_send.at[2], c_recv.at[p]).wait_recv()

        @pl.when(inside)
        def _():
            whole(
                t_buf.at[step, 1:3, :, rows], halo_send.at[step], halo_recv.at[step, p]
            ).wait_recv()

        @pl.when(jnp.logical_not(inside))
        def _():
            whole(
                t_buf.at[step, 1, :, rows], halo_send.at[step], halo_recv.at[step, p]
            ).wait_recv()

    def chunk_rows(i):
        return pl.ds(8 * i, 8) if isinstance(i, int) else pl.ds(pl.multiple_of(i * 8, 8), 8)

    def operate(step, before, finish, extra, meanwhile=None):
        def chunk(i, behind, extra):
            behind = list(behind)
            rows, after = chunk_rows(i), chunk_rows(i + 1)
            stiff, extra = before(rows, extra)
            total = [None, None]
            lower = None
            for n in range(4):
                upper = []
                for c in range(3):
                    v, w = t_buf[step, n, c, rows], t_buf[step, n, c, after]
                    upper.append(plane_modes(v, w, row, col))
                if n:
                    e = n - 1
                    f = cell_forces(cell_modes(lower, upper), stiff[e])
                    for node, sign in ((e, 1.0), (e - 1, -1.0)):
                        if not 0 <= node < 2:
                            continue
                        part = {}
                        for c in range(3):
                            for q in range(4):
                                hi = f[4 + q, c]
                                if q == 0:
                                    value = hi if sign > 0 else -hi
                                else:
                                    value = f[q, c] + hi if sign > 0 else f[q, c] - hi
                                part[c, q] = value
                        if total[node] is None:
                            total[node] = part
                        else:
                            total[node] = {key: total[node][key] + part[key] for key in part}
                lower = upper
            for node in range(2):
                for c in range(3):
                    g = []
                    for px in range(2):
                        fs, fd = total[node][c, 2 * px], total[node][c, 2 * px + 1]
                        shifted = jnp.where(col == 0, 0.0, pltpu.roll(fs + fd, 1, 1))
                        g.append(fs - fd + shifted)
                    r = pltpu.roll(g[0] + g[1], 1, 0)
                    slot = 3 * node + c
                    value = g[0] - g[1] + jnp.where(row == 0, behind[slot], r)
                    behind[slot] = r
                    extra = finish(node, c, rows, value, extra)
            return tuple(behind), extra

        def body(p, carry):
            behind, extra = carry

            @pl.when(p < PIECES - 1)
            def _():
                wait_piece(step, p + 1)

            for part in range(2):
                behind, extra = chunk(2 * p - 2 + part, behind, extra)
            send_piece(step + 1, p)
            return behind, extra

        mark(f"wait{step}")
        wait_piece(step, 0)
        if meanwhile:
            meanwhile()
        mark(f"app{step}")
        behind = (zero8,) * 6
        for p in range(2):
            wait_piece(step, p + 1)
            behind, extra = chunk(p, behind, extra)
            send_piece(step + 1, p)
        return lax.fori_loop(2, PIECES, body, (behind, extra))[1]

    def send_piece(step, p):
        rows = piece(p)
        if step < SWEEPS:
            @pl.when(k < PLANE - 1)
            def _():
                start(
                    t_buf.at[step, 2, :, rows], t_buf.at[step, 0, :, rows],
                    halo_send.at[step], halo_recv.at[step, p], at(above),
                )

        @pl.when(k > 0)
        def _():
            start(
                t_buf.at[step, 1, :, rows], t_buf.at[step, 3, :, rows],
                halo_send.at[step], halo_recv.at[step, p], at(below),
            )

    def stiffness(rows, extra):
        acc, rolls = extra
        stiff = [STIFF_VOID + (1.0 - STIFF_VOID) * c_buf[e, rows] for e in range(3)]
        stiff[0] = stiff[0] * has_below
        out = []
        for e in range(3):
            stiff_buf[e, rows] = stiff[e]
        for n in range(2):
            b = stiff[n] + stiff[n + 1]
            b = b + jnp.where(col == 0, 0.0, pltpu.roll(b, 1, 1))
            r = pltpu.roll(b, 1, 0)
            b = b + jnp.where(row == 0, rolls[n], r)
            out.append(r)
            free = free_buf[n, rows]
            inv_buf[n, rows] = 1.0 / (free * KD * b + (1.0 - free))
        return stiff, (acc, tuple(out))

    def first(n, c, rows, value, extra):
        free, inv = free_buf[n, rows], inv_buf[n, rows]
        r = free * (rhs_buf[n, c, rows] - value) - (1.0 - free) * u0_buf[n, c, rows]
        g = r * inv
        v_buf[0, n, c, rows] = g
        t_buf[1, 1 + n, c, rows] = free * g
        return extra[0] + r * g, extra[1]

    def held(rows, extra):
        return [stiff_buf[e, rows] for e in range(3)], extra

    def later(step):
        def finish(n, c, rows, value, extra):
            free, inv = free_buf[n, rows], inv_buf[n, rows]
            v = v_buf[step - 1, n, c, rows]
            w = free * value + (1.0 - free) * v
            new = w * inv
            v_buf[step, n, c, rows] = new
            t_buf[step + 1, 1 + n, c, rows] = free * new
            return extra + v * w if step == 1 else extra

        return finish

    gr = operate(0, stiffness, first, (zero8, (zero8, zero8)))[0]
    mark("mid0")
    zs.wait_recv()
    z_mix(0)
    ys = y_send(1, 0)
    count8 = zero8
    for n in range(2):
        for i in range(ROWS // 8):
            count8 = count8 + jnp.where(solid_buf[n, 8 * i : 8 * i + 8] > 0.0, 1.0, 0.0)
    gw = operate(1, held, later(1), zero8)

    mark("mid1")
    lane = lax.broadcasted_iota(jnp.int32, (1, COLS), 1)
    line0 = jnp.zeros((1, COLS), F32)
    pl.semaphore_wait(heard.at[1], NY_ - 1)
    for i, tile in enumerate((gr, gw, count8)):
        line0 = jnp.where(lane == i, total_of(tile), line0)
    sz_buf[0] = line0
    scalars = group(2, sz_buf, PLANE, lambda i: sz_buf.at[0], plane_peer)
    ys.wait_recv()
    denom = y_sum(0)
    for a in range(2):
        den_buf[a] = denom[a]
        fz_buf[1, 0, a] = jnp.where(solid_buf[a, mine8] > 0.0, 1.0, 0.0) / denom[a]
    zs = z_send(3, 1)
    operate(2, held, later(2), 0)
    q_flight = []

    def q_mix():
        zs.wait_recv()
        z_mix(1)
        q_flight.append(y_send(5, 1))

    operate(3, held, later(3), 0, q_mix)
    mark("combine")
    scalars.wait_recv()
    line0 = sum_of(sz_buf, PLANE)
    gr_all, gw_all, count = line0[:, 0:1], line0[:, 1:2], line0[:, 2:3]
    coefs = [jnp.broadcast_to(c, (8, COLS)) for c in chebyshev(UPPER_FACTOR * gw_all / gr_all)]

    @pl.loop(0, ROWS // 8)
    def _(i):
        rows = pl.ds(pl.multiple_of(i * 8, 8), 8)
        for n in range(2):
            free = free_buf[n, rows]
            for c in range(3):
                u = u0_buf[n, c, rows]
                for power in range(SWEEPS):
                    u = u + coefs[power] * v_buf[power, n, c, rows]
                send_buf[n, c, rows] = u
                tu_buf[n, c, rows] = free * u

    def own_layer(n, c, rows):
        return tu_buf[n, c, rows]

    def upper_layer(n, c, rows):
        if n < 2:
            return tu_buf[n, c, rows]
        u = t_buf[0, 3, c, rows]
        for power in range(SWEEPS):
            u = u + coefs[power] * t_buf[power + 1, 3, c, rows]
        return u

    def energy_chunk(e, layer, i):
        rows, after = chunk_rows(i), chunk_rows(i + 1)
        planes = [
            [plane_modes(layer(n, c, rows), layer(n, c, after), row, col) for c in range(3)]
            for n in (e, e + 1)
        ]
        value = cell_energy(cell_modes(*planes))
        weight = (3.0 * (1.0 - STIFF_VOID)) * c_buf[1 + e, rows]
        num_buf[e, rows] = weight * value

    def smooth_xy(plane):
        return dot(gauss_x, dot(plane, gauss_y))

    mark("energy0")

    @pl.loop(0, ROWS // 16)
    def _(p):
        for part in range(2):
            energy_chunk(0, own_layer, 2 * p + part)

    rs0 = smooth_xy(num_buf[0])
    mark("wait_last")

    def last_piece(p):
        @pl.when(k < PLANE - 1)
        def _():
            whole(
                t_buf.at[SWEEPS, 3, :, piece(p)], halo_send.at[SWEEPS], halo_recv.at[SWEEPS, p]
            ).wait_recv()

    last_piece(0)
    for p in range(2):
        last_piece(p + 1)
        energy_chunk(1, upper_layer, p)

    @pl.loop(2, PIECES)
    def _(p):
        @pl.when(p < PIECES - 1)
        def _():
            last_piece(p + 1)

        for part in range(2):
            energy_chunk(1, upper_layer, 2 * p - 2 + part)

    mark("smoothn")
    rs1 = smooth_xy(num_buf[1])
    num2_buf[0] = rs0
    num2_buf[1] = rs1
    for a in range(2):
        rs_buf[0, a] = num2_buf[a, mine8]
    xs = group(
        7, rs_buf, RING,
        lambda d: num2_buf.at[:, pl.ds(pl.multiple_of(8 * ring_peer(d)[0], 8), 8)],
        lambda d: ring_peer(d)[1],
    )
    mark("wait_rs")
    xs.wait_recv()
    totals = [sum_of(rs_buf.at[:, a], RING) for a in range(2)]
    for a in range(2):
        fz_buf[2, 0, a] = totals[a]
    zs = z_send(4, 2)
    mark("wpart")
    q_flight[0].wait_recv()
    q8 = y_sum(1)
    wx_buf[0] = jnp.sum(q8[0] * totals[0] + q8[1] * totals[1], axis=0, keepdims=True)
    wxs = group(8, wx_buf, RING, lambda d: wx_buf.at[0], lambda d: ring_peer(d)[1])
    got_back = one(3, send_buf.at[other], back_buf, partner)
    for c in range(3):
        disp_out[h, c, 0] = send_buf[h, c]
    mark("wait_wx")
    wxs.wait_recv()
    wz_buf[0] = sum_of(wx_buf, RING)
    wzs = group(9, wz_buf, PLANE, lambda i: wz_buf.at[0], plane_peer)
    mark("wait_z")
    zs.wait_recv()
    mark("zmix2")
    z_mix(2)
    ys = y_send(6, 2)
    mark("wait_y")
    ys.wait_recv()
    numer = y_sum(2)
    for a in range(2):
        here = jnp.where(solid_buf[a, mine8] > 0.0, 1.0, 0.0)
        xt_buf[0, a] = here * (numer[a] / den_buf[a])
    xs = group(10, xt_buf, RING, lambda d: xt_buf.at[0], lambda d: ring_peer(d)[1])
    mark("wait_wz")
    wzs.wait_recv()
    weighted_all = jnp.sum(sum_of(wz_buf, PLANE), axis=1, keepdims=True)
    inv_mean = 1.0 / (weighted_all / count + EPSILON)
    mark("wait_x")
    xs.wait_recv()
    mark("trial")
    tile = zero8
    for d in range(RING):
        there = pl.ds(pl.multiple_of(8 * lax.rem(j + RING - d, RING), 8), 8)
        for a in range(2):
            old = solid_buf[a, there]
            trial = jnp.minimum(
                jnp.maximum(old * jnp.sqrt(xt_buf[d, a] * inv_mean), old - MOVE_LIMIT),
                old + MOVE_LIMIT,
            )
            tile = tile + trial
            trial_buf[a, there] = trial
    vol_buf[0] = jnp.sum(tile, axis=0, keepdims=True)
    vs = group(11, vol_buf, PLANE, lambda i: vol_buf.at[0], plane_peer)
    mark("wait_back")
    got_back.wait_recv()
    for c in range(3):
        disp_out[other, c, 0] = back_buf[c]
    for copy in sent[:-1]:
        copy.wait_send()

    def layers_sent(step, layers):
        whole(
            t_buf.at[step, layers, :, 0:ROWS], halo_send.at[step], halo_recv.at[step, 0]
        ).wait_send()

    for step in range(SWEEPS):
        pl.when(inside)(lambda: layers_sent(step, pl.ds(1, 2)))
        pl.when(jnp.logical_not(inside))(lambda: layers_sent(step, 1))
    pl.when(k > 0)(lambda: layers_sent(SWEEPS, 1))
    pl.when(k < PLANE - 1)(lambda: whole(c_buf.at[0], one_send.at[2], c_recv.at[0]).wait_send())
    mark("wait_vol")
    vs.wait_recv()
    mark("finish")
    volume = jnp.sum(sum_of(vol_buf, PLANE), axis=1, keepdims=True)
    scale = VOLUME_TARGET / (volume / count + EPSILON)
    dens_out[0] = jnp.minimum(scale * trial_buf[h], 1.0)
    vs.wait_send()
    mark(None)


def put_out(disp_ref, dens_ref, disp_out, dens_out, sems):
    copies = [
        pltpu.make_async_copy(disp_ref, disp_out, sems.at[0]),
        pltpu.make_async_copy(dens_ref, dens_out, sems.at[1]),
    ]
    for copy in copies:
        copy.start()
    for copy in copies:
        copy.wait()


def shards(start_disp, density, design, support, load_nodes, load_forces):
    arrays = (
        start_disp, density, design, support, load_nodes, jnp.transpose(load_forces, (1, 0, 2)),
    )
    vmem = lambda *shape: pltpu.VMEM(shape, F32)
    dma = lambda *shape: pltpu.SemaphoreType.DMA(shape)
    plane = (ROWS, COLS)
    results = pl.pallas_call(
        kernel,
        out_shape=(
            pltpu.VMEM(start_disp.shape, F32),
            pltpu.VMEM(density.shape, F32),
        ),
        in_specs=[pl.BlockSpec(memory_space=pltpu.HBM)] * 6,
        out_specs=(pl.BlockSpec(memory_space=pltpu.VMEM),) * 2,
        scratch_shapes=[
            vmem(1, *plane),
            pltpu.VMEM((1, *plane), jnp.int32),
            pltpu.VMEM((1, *plane), jnp.int32),
            pltpu.VMEM((2, POINTS), jnp.int32),
            vmem(3, 2, POINTS),
            vmem(SWEEPS + 1, 4, 3, ROWS + 8, COLS),
            vmem(SWEEPS, 2, 3, *plane),
            vmem(2, 3, *plane),
            vmem(2, 3, *plane),
            vmem(3, *plane),
            vmem(2, *plane),
            vmem(3, *plane),
            vmem(2, *plane),
            vmem(2, *plane),
            vmem(5, *plane),
            vmem(5, *plane),
            vmem(2, 3, ROWS + 8, COLS),
            vmem(2, 3, *plane),
            vmem(3, *plane),
            vmem(3 * NY_ * NZ_, 8, COLS),
            vmem(8, COLS),
            vmem(8, COLS),
            vmem(3, NZ_, 2, 8, COLS),
            vmem(3, NY_, 2, 8, COLS),
            vmem(3, NY_, 2, 8, COLS),
            vmem(*plane),
            vmem(2, *plane),
            vmem(2, *plane),
            vmem(RING, 2, 8, COLS),
            vmem(RING, 2, 8, COLS),
            vmem(2, *plane),
            vmem(2, 8, COLS),
            vmem(PLANE, 1, COLS),
            vmem(RING, 1, COLS),
            vmem(PLANE, 1, COLS),
            vmem(PLANE, 1, COLS),
            pltpu.SemaphoreType.REGULAR((2,)), dma(7), dma(PIECES), dma(SWEEPS + 1, PIECES), dma(PIECES), dma(SWEEPS + 1),
            dma(4), dma(4), dma(12), dma(12),
        ],
        compiler_params=pltpu.CompilerParams(
            collective_id=0, has_side_effects=True, vmem_limit_bytes=48 * 1024 * 1024
        ),
    )(*(pltpu.with_memory_space_constraint(a, pltpu.HBM) for a in arrays))
    return pl.pallas_call(
        put_out,
        out_shape=(
            pltpu.HBM(start_disp.shape, F32),
            pltpu.HBM(density.shape, F32),
        ),
        in_specs=[pl.BlockSpec(memory_space=pltpu.VMEM)] * 2,
        out_specs=(pl.BlockSpec(memory_space=pltpu.HBM),) * 2,
        scratch_shapes=[dma(2)],
    )(*(pltpu.with_memory_space_constraint(a, pltpu.VMEM) for a in results))


def solution(mesh):
    return jax.shard_map(
        shards,
        mesh=mesh,
        in_specs=(
            P("load", None, "slab", None, None),
            P("slab", None, None),
            P("slab", None, None),
            P("slab", None, None),
            P("load", None),
            P("load", None, None),
        ),
        out_specs=(P("load", None, "slab", None, None), P("slab", None, None)),
        check_vma=False,
    )
```
